32 devices in a mesh: dp: 1 (over z), ing: 4 (over y), grp: 8 (over x, core).
Axes of the slice: x: 4, y: 4, z: 1, core: 2. Of those that a mesh axis runs over, the one named last changes fastest.
The devices are a block of a 4x4x8 slice.
Arguments:
- x_tokens: bfloat16 [32768, 1024], P(('dp', 'grp', 'ing'))
- expert_ids: int32 [32768, 8], P(('dp', 'grp', 'ing'))
- gate_vals: float32 [32768, 8], P(('dp', 'grp', 'ing'))
- y_grad: bfloat16 [32768, 1024], P(('dp', 'grp', 'ing'))
- w_gate: bfloat16 [32, 1024, 512], P(('grp', 'ing'))
- w_up: bfloat16 [32, 1024, 512], P(('grp', 'ing'))
- w_down: bfloat16 [32, 512, 1024], P(('grp', 'ing'))
Outputs:
- output 1: bfloat16 [32768, 1024], P(('dp', 'grp', 'ing'))
- output 2: bfloat16 [32768, 1024], P(('dp', 'grp', 'ing'))
- output 3: float32 [32, 1024, 512], P(('dp', 'grp', 'ing'))
- output 4: float32 [32, 1024, 512], P(('dp', 'grp', 'ing'))
- output 5: float32 [32, 512, 1024], P(('dp', 'grp', 'ing'))
All inputs are finite; a program needn't handle non-finite values.
Results may differ from the reference program's by a relative error of at most 0.00889638.
Values are sent between devices in bfloat16 or wider.
A program may use at most 768 MiB of HBM per device.

```python
import jax
import jax.numpy as jnp
from jax import lax

HIDDEN = 1024
EXPERT_FF = 512
NUM_EXPERTS = 32
TOP_K = 8
TOKENS = 1024
GROUPS = 8
INNER = 4
GROUP_LIMIT = 4

DEVICES = GROUPS * INNER
PER_GROUP = NUM_EXPERTS // GROUPS
PICKS = TOP_K // GROUP_LIMIT
GROUP_SLOTS = TOKENS * GROUP_LIMIT // GROUPS
CAPACITY = 3 * TOKENS * TOP_K // (2 * NUM_EXPERTS)


def draw_routing(dev_key):
    key_rank, key_group, key_expert, key_cols = jax.random.split(dev_key, 4)
    token_rank = jax.random.permutation(key_rank, TOKENS)
    group_perm = jax.random.permutation(key_group, GROUPS)
    expert_perm = jax.vmap(lambda sub_key: jax.random.permutation(sub_key, PER_GROUP))(jax.random.split(key_expert, GROUPS))
    col_perm = jax.vmap(lambda sub_key: jax.random.permutation(sub_key, TOP_K))(jax.random.split(key_cols, TOKENS))
    cycle_pos = token_rank[:, None] * GROUP_LIMIT + jnp.arange(GROUP_LIMIT)[None, :]
    chosen = group_perm[cycle_pos % GROUPS]
    order_in = (cycle_pos // GROUPS)[:, :, None]
    pick_ids = jnp.arange(PICKS)[None, None, :]
    half_slots = GROUP_SLOTS // 2
    wide_pos = (order_in * PICKS + pick_ids) % PER_GROUP
    narrow_pos = ((order_in - half_slots) * PICKS + pick_ids) % (PER_GROUP // 2)
    local_pos = jnp.where(order_in < half_slots, wide_pos, narrow_pos)
    local_ids = expert_perm[chosen[:, :, None], local_pos]
    global_ids = (chosen[:, :, None] * PER_GROUP + local_ids).reshape(TOKENS, TOP_K)
    return jnp.take_along_axis(global_ids, col_perm, axis=1).astype(jnp.int32)


def setup_inputs(seed: int = 0, part: int = 0) -> dict:
    part_key = jax.random.fold_in(jax.random.key(seed), part)
    key_route, key_gate, key_x, key_dy = jax.random.split(part_key, 4)
    route_keys = jax.random.split(key_route, DEVICES)
    expert_ids = jax.vmap(draw_routing)(route_keys).reshape(DEVICES * TOKENS, TOP_K)
    raw_gate = jnp.exp(0.5 * jax.random.normal(key_gate, (DEVICES * TOKENS, TOP_K), jnp.float32))
    gate_vals = raw_gate / jnp.sum(raw_gate, axis=1, keepdims=True)
    x_tokens = jax.random.normal(key_x, (DEVICES * TOKENS, HIDDEN), jnp.float32).astype(jnp.bfloat16)
    y_grad = jax.random.normal(key_dy, (DEVICES * TOKENS, HIDDEN), jnp.float32).astype(jnp.bfloat16)
    key_wg, key_wu, key_wd = jax.random.split(jax.random.key(seed + 1), 3)
    w_gate = (jax.random.normal(key_wg, (NUM_EXPERTS, HIDDEN, EXPERT_FF), jnp.float32) * HIDDEN ** -0.5).astype(jnp.bfloat16)
    w_up = (jax.random.normal(key_wu, (NUM_EXPERTS, HIDDEN, EXPERT_FF), jnp.float32) * HIDDEN ** -0.5).astype(jnp.bfloat16)
    w_down = (jax.random.normal(key_wd, (NUM_EXPERTS, EXPERT_FF, HIDDEN), jnp.float32) * EXPERT_FF ** -0.5).astype(jnp.bfloat16)
    return {'x_tokens': x_tokens, 'expert_ids': expert_ids, 'gate_vals': gate_vals, 'y_grad': y_grad, 'w_gate': w_gate, 'w_up': w_up, 'w_down': w_down}


def reference(x_tokens, expert_ids, gate_vals, y_grad, w_gate, w_up, w_down):
    total_tok = x_tokens.shape[0]
    slot_count = DEVICES * CAPACITY
    flat_ids = expert_ids.reshape(-1)
    flat_gates = gate_vals.reshape(-1)
    pair_order = jnp.argsort(flat_ids, stable=True).astype(jnp.int32)
    counts = jnp.bincount(flat_ids, length=NUM_EXPERTS)
    starts = jnp.cumsum(counts) - counts
    padded_order = jnp.concatenate([pair_order, jnp.zeros((slot_count,), jnp.int32)])
    zero_acc = jnp.zeros((total_tok, HIDDEN), jnp.float32)

    def expert_step(acc_pair, expert):
        part_y, part_dx = acc_pair
        pair_ids = lax.dynamic_slice(padded_order, (starts[expert],), (slot_count,))
        is_valid = jnp.arange(slot_count) < counts[expert]
        tok_rows = pair_ids // TOP_K
        slot_gate = jnp.where(is_valid, flat_gates[pair_ids], 0.0)
        xs_rows = x_tokens[tok_rows]
        dy_rows = y_grad[tok_rows]
        h_gate = jnp.dot(xs_rows, w_gate[expert], preferred_element_type=jnp.float32)
        h_up = jnp.dot(xs_rows, w_up[expert], preferred_element_type=jnp.float32)
        sig_gate = jax.nn.sigmoid(h_gate)
        silu_gate = h_gate * sig_gate
        act_bf = (silu_gate * h_up).astype(jnp.bfloat16)
        out_bf = jnp.dot(act_bf, w_down[expert], preferred_element_type=jnp.float32).astype(jnp.bfloat16)
        d_out = (slot_gate[:, None] * dy_rows.astype(jnp.float32)).astype(jnp.bfloat16)
        d_act = jnp.dot(d_out, w_down[expert].T, preferred_element_type=jnp.float32)
        d_hgate = (d_act * h_up * sig_gate * (1.0 + h_gate * (1.0 - sig_gate))).astype(jnp.bfloat16)
        d_hup = (d_act * silu_gate).astype(jnp.bfloat16)
        dx_rows = (jnp.dot(d_hgate, w_gate[expert].T, preferred_element_type=jnp.float32) + jnp.dot(d_hup, w_up[expert].T, preferred_element_type=jnp.float32)).astype(jnp.bfloat16)
        part_y = part_y.at[tok_rows].add(slot_gate[:, None] * out_bf.astype(jnp.float32))
        part_dx = part_dx.at[tok_rows].add(dx_rows.astype(jnp.float32))
        grad_gate = jnp.dot(xs_rows.T, d_hgate, preferred_element_type=jnp.float32)
        grad_up = jnp.dot(xs_rows.T, d_hup, preferred_element_type=jnp.float32)
        grad_down = jnp.dot(act_bf.T, d_out, preferred_element_type=jnp.float32)
        return (part_y, part_dx), (grad_gate, grad_up, grad_down)

    def group_step(acc_pair, group_id):
        y_acc, dx_acc = acc_pair
        expert_list = group_id * PER_GROUP + jnp.arange(PER_GROUP)
        (part_y, part_dx), grad_stack = lax.scan(expert_step, (zero_acc, zero_acc), expert_list)
        y_acc = y_acc + part_y.astype(jnp.bfloat16).astype(jnp.float32)
        dx_acc = dx_acc + part_dx.astype(jnp.bfloat16).astype(jnp.float32)
        return (y_acc, dx_acc), grad_stack

    (y_acc, dx_acc), grad_stack = lax.scan(group_step, (zero_acc, zero_acc), jnp.arange(GROUPS))
    grad_gate, grad_up, grad_down = grad_stack
    return (y_acc.astype(jnp.bfloat16), dx_acc.astype(jnp.bfloat16), grad_gate.reshape(NUM_EXPERTS, HIDDEN, EXPERT_FF), grad_up.reshape(NUM_EXPERTS, HIDDEN, EXPERT_FF), grad_down.reshape(NUM_EXPERTS, EXPERT_FF, HIDDEN))
```

```python
import functools

import jax
import jax.numpy as jnp
from jax import lax
from jax.experimental import pallas as pl
from jax.experimental.pallas import tpu as pltpu
from jax.sharding import PartitionSpec as P

F32 = jnp.float32
BF16 = jnp.bfloat16
SUB = 128
TILE = 256


def dot(a, b, ca, cb):
    return lax.dot_general(a, b, (((ca,), (cb,)), ((), ())), preferred_element_type=F32)


def split3(v):
    hi = v.astype(BF16)
    rest = v - hi.astype(F32)
    mid = rest.astype(BF16)
    lo = (rest - mid.astype(F32)).astype(BF16)
    return jnp.concatenate([hi.astype(F32), mid.astype(F32), lo.astype(F32)], axis=0).astype(BF16)


def pack_kernel(groups, per_group, cap, ids_ref, gates_ref, x_ref, dy_ref, packed_ref, meta_ref, slot_ref, slots, vals):
    h = pl.program_id(0)
    top_k, tokens = ids_ref.shape
    num_exp = groups * per_group

    @pl.when(h == 0)
    def _():
        exp_iota = lax.broadcasted_iota(jnp.int32, (num_exp, tokens), 0)
        grp_iota = lax.broadcasted_iota(jnp.int32, (groups, tokens), 0)
        mem = jnp.zeros((num_exp, tokens), F32)
        gate = jnp.zeros((num_exp, tokens), F32)
        gmem = jnp.zeros((groups, tokens), F32)
        for j in range(top_k):
            row = ids_ref[j:j + 1, :]
            hit = row == exp_iota
            mem = jnp.where(hit, 1.0, mem)
            gate = jnp.where(hit, gates_ref[j:j + 1, :], gate)
            gmem = jnp.where((row // per_group) == grp_iota, 1.0, gmem)
        upper = (lax.broadcasted_iota(jnp.int32, (tokens, tokens), 0) <= lax.broadcasted_iota(jnp.int32, (tokens, tokens), 1)).astype(F32).astype(BF16)
        rank = jnp.where(mem > 0, dot(mem.astype(BF16), upper, 1, 0), 0.0)
        slot = jnp.where(gmem > 0, dot(gmem.astype(BF16), upper, 1, 0), 0.0)
        slots[...] = slot
        slot_ref[...] = slot
        for g in range(groups):
            vals[g, 0:per_group, :] = rank[g * per_group:(g + 1) * per_group, :]
            vals[g, per_group:2 * per_group, :] = gate[g * per_group:(g + 1) * per_group, :]

    row = slots[pl.ds(h, 1), :]
    pick = (row == (lax.broadcasted_iota(jnp.int32, (cap, tokens), 0) + 1).astype(F32)).astype(F32).astype(BF16)
    hidden = x_ref.shape[1]
    packed_ref[0, :, 0:hidden] = dot(pick, x_ref[...], 1, 0).astype(BF16)
    packed_ref[0, :, hidden:] = dot(pick, dy_ref[...], 1, 0).astype(BF16)
    parts = dot(split3(vals[h]), pick, 1, 1)
    n = 2 * per_group
    meta_ref[0] = (parts[0:n] + parts[n:2 * n]) + parts[2 * n:3 * n]


def pack_rows(ids_t, gates_t, x, dy, groups, per_group, cap):
    top_k, tokens = ids_t.shape
    hidden = x.shape[1]
    whole = lambda shape: pl.BlockSpec(shape, lambda h: (0,) * len(shape))
    return pl.pallas_call(
        functools.partial(pack_kernel, groups, per_group, cap),
        grid=(groups,),
        out_shape=(
            jax.ShapeDtypeStruct((groups, cap, 2 * hidden), BF16),
            jax.ShapeDtypeStruct((groups, 2 * per_group, cap), F32),
            jax.ShapeDtypeStruct((groups, tokens), F32),
        ),
        in_specs=[whole((top_k, tokens)), whole((top_k, tokens)), whole((tokens, hidden)), whole((tokens, hidden))],
        out_specs=(
            pl.BlockSpec((1, cap, 2 * hidden), lambda h: (h, 0, 0)),
            pl.BlockSpec((1, 2 * per_group, cap), lambda h: (h, 0, 0)),
            whole((groups, tokens)),
        ),
        scratch_shapes=[pltpu.VMEM((groups, tokens), F32), pltpu.VMEM((groups, 2 * per_group, tokens), F32)],
        compiler_params=pltpu.CompilerParams(vmem_limit_bytes=48 * 1024 * 1024),
        cost_estimate=pl.CostEstimate(flops=4 * groups * cap * tokens * hidden, bytes_accessed=groups * cap * hidden * 4, transcendentals=0),
        name='pack_rows',
    )(ids_t, gates_t, x, dy)


def expert_kernel(max_tiles, has_prev, cnt_ref, *refs):
    meta_ref, xd_ref, w1_ref, w3_ref, w2_ref = refs[:5]
    refs = refs[5:]
    prev = refs[:3] if has_prev else None
    refs = refs[3:] if has_prev else refs
    pq_ref, g1_ref, g3_ref, g2_ref, buf, pq, acc1, acc3, acc2, stage, in_sem, out_sem, pq_sem = refs
    k = pl.program_id(0)
    per_group = pl.num_programs(0)
    srcs, rows2, cap = meta_ref.shape
    hidden = xd_ref.shape[2] // 2
    accs = (acc1, acc3, acc2)
    outs = (g1_ref, g3_ref, g2_ref)

    @pl.when(k > 0)
    def _():
        for i in range(3):
            pltpu.make_async_copy(accs[i], outs[i].at[k - 1], out_sem.at[i]).wait()

    if has_prev:
        for i in range(3):
            pltpu.make_async_copy(prev[i].at[k], accs[i], in_sem.at[i]).start()
    else:
        for a in accs:
            a[...] = jnp.zeros_like(a)

    @pl.when(k == 0)
    def _():
        pq[...] = jnp.zeros_like(pq)

    def pick(s, m):
        slot = (lax.broadcasted_iota(jnp.int32, (m, cap), 0) + 1).astype(F32)
        return meta_ref[s, pl.ds(k, 1), :] == slot

    offs = []
    off = jnp.int32(0)
    for s in range(srcs):
        tiles = (cnt_ref[s, k] + SUB - 1) // SUB
        offs.append((pl.multiple_of(off, SUB), tiles))
        off = off + tiles * SUB
    total = off

    for s in range(srcs):
        start, tiles = offs[s]
        for t in range(1, max_tiles + 1):
            m = t * SUB

            @pl.when(tiles == t)
            def _(s=s, m=m, start=start):
                hit = pick(s, m)
                sel = hit.astype(F32).astype(BF16)
                buf[pl.ds(start, m), 0:hidden] = dot(sel, xd_ref[s, :, 0:hidden], 1, 0).astype(BF16)
                gate = jnp.sum(jnp.where(hit, meta_ref[s, pl.ds(per_group + k, 1), :], 0.0), axis=1, keepdims=True)
                buf[pl.ds(start, m), hidden:] = (gate * dot(sel, xd_ref[s, :, hidden:], 1, 0)).astype(BF16)

    n_tiles = (total + TILE - 1) // TILE

    @pl.loop(total // SUB, n_tiles * (TILE // SUB))
    def _(i):
        buf[pl.ds(pl.multiple_of(i * SUB, SUB), SUB), :] = jnp.zeros((SUB, 2 * hidden), BF16)

    if has_prev:
        for i in range(3):
            pltpu.make_async_copy(prev[i].at[k], accs[i], in_sem.at[i]).wait()

    @pl.loop(0, n_tiles)
    def _(i):
        r0 = pl.multiple_of(i * TILE, TILE)
        x = buf[pl.ds(r0, TILE), 0:hidden]
        d = buf[pl.ds(r0, TILE), hidden:]
        h1 = dot(x, w1_ref[0], 1, 0)
        h3 = dot(x, w3_ref[0], 1, 0)
        da = dot(d, w2_ref[0], 1, 1)
        sig = jax.nn.sigmoid(h1)
        silu = h1 * sig
        a = (silu * h3).astype(BF16)
        dh1 = (da * h3 * sig * (1.0 + h1 * (1.0 - sig))).astype(BF16)
        dh3 = (da * silu).astype(BF16)
        acc1[...] += dot(x, dh1, 0, 0)
        acc3[...] += dot(x, dh3, 0, 0)
        acc2[...] += dot(a, d, 0, 0)
        buf[pl.ds(r0, TILE), 0:hidden] = dot(a, w2_ref[0], 1, 0).astype(BF16)
        buf[pl.ds(r0, TILE), hidden:] = (dot(dh1, w1_ref[0], 1, 1) + dot(dh3, w3_ref[0], 1, 1)).astype(BF16)

    for i in range(3):
        pltpu.make_async_copy(accs[i], outs[i].at[k], out_sem.at[i]).start()

    for s in range(srcs):
        start, tiles = offs[s]
        for t in range(1, max_tiles + 1):
            m = t * SUB

            @pl.when(tiles == t)
            def _(s=s, m=m, start=start):
                sel = pick(s, m).astype(F32).astype(BF16)
                cols = jnp.transpose(meta_ref[s])
                lane = lax.broadcasted_iota(jnp.int32, (cap, rows2), 1)
                gate = jnp.sum(jnp.where(lane == per_group + k, cols, 0.0), axis=1, keepdims=True)
                pq[s, :, 0:hidden] += gate * dot(sel, buf[pl.ds(start, m), 0:hidden], 0, 0)
                pq[s, :, hidden:] += dot(sel, buf[pl.ds(start, m), hidden:], 0, 0)

    @pl.when(k == per_group - 1)
    def _():
        for s in range(srcs):
            slot = s % 2
            if s >= 2:
                pltpu.make_async_copy(stage.at[slot], pq_ref.at[s - 2], pq_sem.at[slot]).wait()
            stage[slot] = pq[s].astype(BF16)
            pltpu.make_async_copy(stage.at[slot], pq_ref.at[s], pq_sem.at[slot]).start()
        for s in range(max(0, srcs - 2), srcs):
            pltpu.make_async_copy(stage.at[s % 2], pq_ref.at[s], pq_sem.at[s % 2]).wait()
        for i in range(3):
            pltpu.make_async_copy(accs[i], outs[i].at[k], out_sem.at[i]).wait()


def run_experts(counts, meta, xd, w1, w3, w2, prev, exp_cap):
    srcs, rows2, cap = meta.shape
    per_group, hidden, ff = w1.shape
    max_tiles = -(-exp_cap // SUB)
    buf_rows = -(-srcs * max_tiles * SUB // TILE) * TILE
    any_spec = pl.BlockSpec(memory_space=pl.ANY)
    vmem = pl.BlockSpec(memory_space=pltpu.VMEM)
    w_spec = lambda a: pl.BlockSpec((1,) + a.shape[1:], lambda k, *_: (k, 0, 0))
    has_prev = prev is not None
    grads = (
        jax.ShapeDtypeStruct(w1.shape, F32),
        jax.ShapeDtypeStruct(w3.shape, F32),
        jax.ShapeDtypeStruct(w2.shape, F32),
    )
    rows = srcs * exp_cap * per_group * 2 // 3
    return pl.pallas_call(
        functools.partial(expert_kernel, max_tiles, has_prev),
        grid_spec=pltpu.PrefetchScalarGridSpec(
            num_scalar_prefetch=1,
            grid=(per_group,),
            in_specs=[vmem, vmem, w_spec(w1), w_spec(w3), w_spec(w2)] + [any_spec] * (3 if has_prev else 0),
            out_specs=[any_spec] * 4,
            scratch_shapes=[
                pltpu.VMEM((buf_rows, 2 * hidden), BF16),
                pltpu.VMEM((srcs, cap, 2 * hidden), F32),
                pltpu.VMEM((hidden, ff), F32),
                pltpu.VMEM((hidden, ff), F32),
                pltpu.VMEM((ff, hidden), F32),
                pltpu.VMEM((2, cap, 2 * hidden), BF16),
                pltpu.SemaphoreType.DMA((3,)),
                pltpu.SemaphoreType.DMA((3,)),
                pltpu.SemaphoreType.DMA((2,)),
            ],
        ),
        out_shape=(jax.ShapeDtypeStruct(xd.shape, BF16),) + grads,
        input_output_aliases={6: 1, 7: 2, 8: 3} if has_prev else {},
        compiler_params=pltpu.CompilerParams(vmem_limit_bytes=63 * 1024 * 1024, dimension_semantics=('arbitrary',)),
        cost_estimate=pl.CostEstimate(flops=rows * (18 * hidden * ff + 8 * cap * hidden), bytes_accessed=srcs * cap * hidden * 8, transcendentals=0),
        name='run_experts',
    )(counts, meta, xd, w1, w3, w2, *(prev or ()))


def home_kernel(slot_ref, ret_ref, y_ref, dx_ref):
    groups, cap, width = ret_ref.shape
    rows = y_ref.shape[0]
    acc = None
    for g in range(groups):
        pick = (slot_ref[g:g + 1, :] == (lax.broadcasted_iota(jnp.int32, (cap, rows), 0) + 1).astype(F32)).astype(F32).astype(BF16)
        part = dot(pick, ret_ref[g], 0, 0)
        acc = part if acc is None else acc + part
    y_ref[...] = acc[:, :width // 2].astype(BF16)
    dx_ref[...] = acc[:, width // 2:].astype(BF16)


def home_sum(slot, ret, block):
    groups, tokens = slot.shape
    _, cap, width = ret.shape
    out = jax.ShapeDtypeStruct((tokens, width // 2), BF16)
    return pl.pallas_call(
        home_kernel,
        grid=(tokens // block,),
        out_shape=(out, out),
        in_specs=[pl.BlockSpec((groups, block), lambda i: (0, i)), pl.BlockSpec(memory_space=pltpu.VMEM)],
        out_specs=(pl.BlockSpec((block, width // 2), lambda i: (i, 0)),) * 2,
        compiler_params=pltpu.CompilerParams(vmem_limit_bytes=48 * 1024 * 1024),
        cost_estimate=pl.CostEstimate(flops=2 * groups * cap * tokens * width, bytes_accessed=groups * cap * width * 2, transcendentals=0),
        name='home_sum',
    )(slot, ret)


def solution(mesh):
    groups = mesh.shape['grp']
    inner = mesh.shape['ing']
    tok_spec = P(('dp', 'grp', 'ing'), None)
    weight_spec = P(('grp', 'ing'), None, None)
    grad_spec = P(('dp', 'grp', 'ing'), None, None)

    def device_fn(x_loc, ids_loc, gates_loc, dy_loc, wg_loc, wu_loc, wd_loc):
        tokens, hidden = x_loc.shape
        top_k = ids_loc.shape[1]
        per_group = wg_loc.shape[0] * inner
        num_exp = per_group * groups
        group_limit = min(max(1, groups // 2), top_k // 2)
        cap = tokens * group_limit // groups
        exp_cap = 3 * tokens * top_k // (2 * num_exp)
        gather = lambda w: lax.all_gather(w, 'ing', axis=0, tiled=True)
        w1, w3, w2 = gather(wg_loc), gather(wu_loc), gather(wd_loc)
        packed, meta, slot = pack_rows(ids_loc.T, gates_loc.T, x_loc, dy_loc, groups, per_group, cap)
        swap = lambda a: lax.all_to_all(a, 'grp', 0, 0, tiled=True)
        recv_meta = swap(meta)
        recv = swap(packed)
        counts = jnp.max(recv_meta[:, :per_group, :], axis=2).astype(jnp.int32)
        half = groups // 2
        grads = None
        outs = []
        for c in range(2):
            sl = slice(c * half, (c + 1) * half)
            res = run_experts(counts[sl], recv_meta[sl], recv[sl], w1, w3, w2, grads, exp_cap)
            outs.append(res[0])
            grads = res[1:]
        ret = swap(jnp.concatenate(outs, axis=0))
        g1, g3, g2 = [lax.psum_scatter(g, 'ing', scatter_dimension=0, tiled=True) for g in grads]
        y_out, dx_out = home_sum(slot, ret, 256)
        return y_out, dx_out, g1, g3, g2

    return jax.shard_map(device_fn, mesh=mesh, in_specs=(tok_spec, tok_spec, tok_spec, tok_spec, weight_spec, weight_spec, weight_spec), out_specs=(tok_spec, tok_spec, grad_spec, grad_spec, grad_spec), check_vma=False)
```

```python
import functools

import jax
import jax.numpy as jnp
from jax import lax
from jax.experimental import pallas as pl
from jax.experimental.pallas import tpu as pltpu
from jax.sharding import PartitionSpec as P


F32 = jnp.float32
BF16 = jnp.bfloat16
ALIGN = 16
TILE = 256


def dot(a, b, ca, cb):
    return lax.dot_general(a, b, (((ca,), (cb,)), ((), ())), preferred_element_type=F32)


def split3(v):
    hi = v.astype(BF16)
    rest = v - hi.astype(F32)
    mid = rest.astype(BF16)
    lo = (rest - mid.astype(F32)).astype(BF16)
    return jnp.concatenate([hi.astype(F32), mid.astype(F32), lo.astype(F32)], axis=0).astype(BF16)


def table_rows(groups, per_group, ids_ref, gates_ref, slots, vals):
    top_k, tokens = ids_ref.shape
    num_exp = groups * per_group
    exp_iota = lax.broadcasted_iota(jnp.int32, (num_exp, tokens), 0)
    grp_iota = lax.broadcasted_iota(jnp.int32, (groups, tokens), 0)
    mem = jnp.zeros((num_exp, tokens), F32)
    gate = jnp.zeros((num_exp, tokens), F32)
    gmem = jnp.zeros((groups, tokens), F32)
    for j in range(top_k):
        row = ids_ref[j:j + 1, :]
        hit = row == exp_iota
        mem = jnp.where(hit, 1.0, mem)
        gate = jnp.where(hit, gates_ref[j:j + 1, :], gate)
        gmem = jnp.where((row // per_group) == grp_iota, 1.0, gmem)
    upper = (lax.broadcasted_iota(jnp.int32, (tokens, tokens), 0) <= lax.broadcasted_iota(jnp.int32, (tokens, tokens), 1)).astype(F32).astype(BF16)
    rank = jnp.where(mem > 0, dot(mem.astype(BF16), upper, 1, 0), 0.0)
    slots[...] = jnp.where(gmem > 0, dot(gmem.astype(BF16), upper, 1, 0), 0.0)
    for g in range(groups):
        vals[g, 0:per_group, :] = rank[g * per_group:(g + 1) * per_group, :]
        vals[g, per_group:2 * per_group, :] = gate[g * per_group:(g + 1) * per_group, :]


def pick_rows(slot_row, first, count):
    want = (lax.broadcasted_iota(jnp.int32, (count, slot_row.shape[1]), 0) + (first + 1)).astype(F32)
    return (slot_row == want).astype(F32).astype(BF16)


def table_kernel(groups, per_group, size, ids_ref, gates_ref, slot_ref, meta_ref, vals):
    table_rows(groups, per_group, ids_ref, gates_ref, slot_ref, vals)
    n = 2 * per_group
    is_rank = lax.broadcasted_iota(jnp.int32, (n, 1), 0) < per_group

    @pl.loop(0, groups)
    def _(h):
        row = slot_ref[pl.ds(h, 1), :]
        split = split3(vals[h])
        base = jnp.zeros((n, 1), F32)
        for c in range(meta_ref.shape[2] // size):
            parts = dot(split, pick_rows(row, c * size, size), 1, 1)
            full = (parts[0:n] + parts[n:2 * n]) + parts[2 * n:3 * n]
            meta_ref[h, :, c * size:(c + 1) * size] = jnp.where(is_rank & (full > 0), full - base, full)
            base = jnp.where(is_rank, jnp.maximum(base, jnp.max(full, axis=1, keepdims=True)), 0.0)


def make_tables(ids_t, gates_t, groups, per_group, cap, size):
    tokens = ids_t.shape[1]
    vmem = pl.BlockSpec(memory_space=pltpu.VMEM)
    return pl.pallas_call(
        functools.partial(table_kernel, groups, per_group, size),
        out_shape=(jax.ShapeDtypeStruct((groups, tokens), F32), jax.ShapeDtypeStruct((groups, 2 * per_group, cap), F32)),
        in_specs=[vmem, vmem],
        out_specs=(vmem, vmem),
        scratch_shapes=[pltpu.VMEM((groups, 2 * per_group, tokens), F32)],
        cost_estimate=pl.CostEstimate(flops=2 * groups * cap * tokens * 128, bytes_accessed=groups * cap * 64, transcendentals=0),
        name='make_tables',
    )(ids_t, gates_t)


def pack_kernel(first, slot_ref, x_ref, dy_ref, packed_ref):
    size, width = packed_ref.shape[1:]
    pick = pick_rows(slot_ref[pl.ds(pl.program_id(0), 1), :], first, size)
    packed_ref[0, :, 0:width // 2] = dot(pick, x_ref[...], 1, 0).astype(BF16)
    packed_ref[0, :, width // 2:] = dot(pick, dy_ref[...], 1, 0).astype(BF16)


def pack_rows(slot, x, dy, c, size):
    groups, tokens = slot.shape
    hidden = x.shape[1]
    vmem = pl.BlockSpec(memory_space=pltpu.VMEM)
    return pl.pallas_call(
        functools.partial(pack_kernel, c * size),
        grid=(groups,),
        out_shape=jax.ShapeDtypeStruct((groups, size, 2 * hidden), BF16),
        in_specs=[vmem, vmem, vmem],
        out_specs=pl.BlockSpec((1, size, 2 * hidden), lambda h: (h, 0, 0)),
        compiler_params=pltpu.CompilerParams(vmem_limit_bytes=58 * 1024 * 1024),
        cost_estimate=pl.CostEstimate(flops=4 * groups * size * tokens * hidden, bytes_accessed=groups * size * hidden * 4, transcendentals=0),
        name='pack_rows',
    )(slot, x, dy)


def grad_parts(hidden, ff):
    mid = hidden + ff // 2
    return (
        (pl.ds(0, hidden), pl.ds(0, ff)),
        (pl.ds(0, hidden), pl.ds(ff, ff)),
        (pl.ds(hidden, ff // 2), pl.ds(0, hidden)),
        (pl.ds(mid, ff // 2), pl.ds(0, hidden)),
    )


def expert_kernel(chunk, first_pos, steps, has_prev, carry_in, carry_out, split, order_ref, meta_ref, xd_ref, w_ref, *refs):
    refs = list(refs)
    prev = refs.pop(0) if has_prev else None
    carried = refs.pop(0) if carry_in else None
    rows_ref = refs.pop(0)
    grad_refs = [refs.pop(0) for _ in range(4 * steps if split else 1)]
    buf, acc, offs, in_sem, out_sem, row_sem = refs[:6]
    pq, stage, pq_sem = (None,) * 3 if carry_out else refs[6:]
    step = pl.program_id(0)
    k = order_ref[first_pos + step]
    srcs, size, width = xd_ref.shape
    hidden = width // 2
    rows2 = meta_ref.shape[1]
    per_group = rows2 // 2
    ff = acc.shape[0] - hidden
    lanes = pl.ds(chunk * size, size)

    def each_grad(at, act):
        if not split:
            act(pltpu.make_async_copy(acc, grad_refs[0].at[at], out_sem.at[0]))
            return
        for i in range(steps):
            @pl.when(at == i)
            def _(i=i):
                for j, (rows, cols) in enumerate(grad_parts(hidden, ff)):
                    act(pltpu.make_async_copy(acc.at[rows, cols], grad_refs[4 * i + j], out_sem.at[j]))

    def load_prev():
        return pltpu.make_async_copy(prev.at[first_pos + step], acc, in_sem)

    @pl.when(step > 0)
    def _():
        each_grad(step - 1, lambda copy: copy.wait())

    if has_prev:
        load_prev().start()
    else:
        acc[...] = jnp.zeros_like(acc)

    def pick(s, k):
        slot = (lax.broadcasted_iota(jnp.int32, (size, size), 0) + 1).astype(F32)
        return meta_ref[s, pl.ds(k, 1), lanes] == slot

    def place(s, k, off):
        offs[s] = off
        count = jnp.max(meta_ref[s, pl.ds(k, 1), lanes]).astype(jnp.int32)
        return off + (count + ALIGN - 1) // ALIGN * ALIGN

    def combine(k, first):
        @pl.loop(0, srcs)
        def _(s):
            off = pl.multiple_of(offs[s], ALIGN)
            sel = pick(s, k).astype(F32).astype(BF16)
            cols = jnp.transpose(meta_ref[s, :, lanes])
            lane = lax.broadcasted_iota(jnp.int32, (size, rows2), 1)
            gate = jnp.sum(jnp.where(lane == per_group + k, cols, 0.0), axis=1, keepdims=True)
            p = gate * dot(sel, buf[pl.ds(off, size), 0:hidden], 0, 0)
            q = dot(sel, buf[pl.ds(off, size), hidden:], 0, 0)
            if first:
                pq[s, :, 0:hidden] = p
                pq[s, :, hidden:] = q
            else:
                pq[s, :, 0:hidden] += p
                pq[s, :, hidden:] += q

    if carry_in:
        @pl.when(step == 0)
        def _():
            copy = pltpu.make_async_copy(carried, buf, row_sem)
            copy.start()
            before = order_ref[first_pos - 1]
            lax.fori_loop(0, srcs, lambda s, off: place(s, before, off), jnp.int32(0))
            copy.wait()
            combine(before, True)

    def gather(s, off):
        off = pl.multiple_of(off, ALIGN)
        hit = pick(s, k)
        sel = hit.astype(F32).astype(BF16)
        gate = jnp.sum(jnp.where(hit, meta_ref[s, pl.ds(per_group + k, 1), lanes], 0.0), axis=1, keepdims=True)
        buf[pl.ds(off, size), 0:hidden] = dot(sel, xd_ref[s, :, 0:hidden], 1, 0).astype(BF16)
        buf[pl.ds(off, size), hidden:] = (gate * dot(sel, xd_ref[s, :, hidden:], 1, 0)).astype(BF16)
        return place(s, k, off)

    total = pl.multiple_of(lax.fori_loop(0, srcs, gather, jnp.int32(0)), ALIGN)
    buf[pl.ds(total, TILE), :] = jnp.zeros((TILE, width), BF16)
    if has_prev:
        load_prev().wait()

    def run(r0, rows):
        x = buf[pl.ds(r0, rows), 0:hidden]
        d = buf[pl.ds(r0, rows), hidden:]
        h = dot(x, w_ref[0, 0:hidden, :], 1, 0)
        da = dot(d, w_ref[0, hidden:, :], 1, 1)
        h1 = h[:, 0:ff]
        h3 = h[:, ff:]
        sig = jax.nn.sigmoid(h1)
        silu = h1 * sig
        a = (silu * h3).astype(BF16)
        dh1 = (da * h3 * sig * (1.0 + h1 * (1.0 - sig))).astype(BF16)
        dh3 = (da * silu).astype(BF16)
        dh = jnp.concatenate([dh1, dh3], axis=1)
        acc[0:hidden, :] += dot(x, dh, 0, 0)
        acc[hidden:, :] += dot(a, d, 0, 0)
        buf[pl.ds(r0, rows), 0:hidden] = dot(a, w_ref[0, hidden:, :], 1, 0).astype(BF16)
        buf[pl.ds(r0, rows), hidden:] = dot(dh, w_ref[0, 0:hidden, :], 1, 1).astype(BF16)

    units = (total + TILE // 2 - 1) // (TILE // 2)

    @pl.loop(0, units // 2)
    def _(i):
        run(pl.multiple_of(i * TILE, TILE), TILE)

    @pl.when(units % 2 == 1)
    def _():
        run(pl.multiple_of((units - 1) * (TILE // 2), TILE // 2), TILE // 2)

    each_grad(step, lambda copy: copy.start())

    if carry_out:
        copy = pltpu.make_async_copy(buf, rows_ref, row_sem)
        copy.start()
        copy.wait()
    elif carry_in:
        combine(k, False)
    else:
        @pl.when(step == 0)
        def _():
            combine(k, True)

        @pl.when(step > 0)
        def _():
            combine(k, False)

    @pl.when(step == steps - 1)
    def _():
        if not carry_out:
            for s in range(srcs):
                slot = s % 2
                if s >= 2:
                    pltpu.make_async_copy(stage.at[slot], rows_ref.at[s - 2], pq_sem.at[slot]).wait()
                stage[slot] = pq[s].astype(BF16)
                pltpu.make_async_copy(stage.at[slot], rows_ref.at[s], pq_sem.at[slot]).start()
            for s in range(max(0, srcs - 2), srcs):
                pltpu.make_async_copy(stage.at[s % 2], rows_ref.at[s], pq_sem.at[s % 2]).wait()
        each_grad(step, lambda copy: copy.wait())


def run_experts(chunk, order, positions, meta, xd, w, prev=None, carried=None, carry_out=False, split=False):
    srcs, size, width = xd.shape
    _, rows, hidden = w.shape
    first, steps = positions[0], len(positions)
    any_spec = pl.BlockSpec(memory_space=pl.ANY)
    vmem = pl.BlockSpec(memory_space=pltpu.VMEM)
    buf_rows = srcs * size + max(size, TILE)
    extra = [a for a in (prev, carried) if a is not None]
    n = srcs * size // 2
    if split:
        parts = grad_parts(hidden, rows - hidden)
        grads = [jax.ShapeDtypeStruct((r.size, c.size), F32) for _ in range(steps) for r, c in parts]
    else:
        grads = [jax.ShapeDtypeStruct((steps, rows, hidden), F32)]
    scratch = [
        pltpu.VMEM((buf_rows, width), BF16),
        pltpu.VMEM((rows, hidden), F32),
        pltpu.SMEM((srcs,), jnp.int32),
        pltpu.SemaphoreType.DMA,
        pltpu.SemaphoreType.DMA((4,)),
        pltpu.SemaphoreType.DMA,
    ]
    if not carry_out:
        scratch += [pltpu.VMEM((srcs, size, width), F32), pltpu.VMEM((2, size, width), BF16), pltpu.SemaphoreType.DMA((2,))]
    return pl.pallas_call(
        functools.partial(expert_kernel, chunk, first, steps, prev is not None, carried is not None, carry_out, split),
        grid_spec=pltpu.PrefetchScalarGridSpec(
            num_scalar_prefetch=1,
            grid=(steps,),
            in_specs=[vmem, vmem, pl.BlockSpec((1, rows, hidden), lambda k, o: (o[first + k], 0, 0))] + [any_spec] * len(extra),
            out_specs=[any_spec] * (1 + len(grads)),
            scratch_shapes=scratch,
        ),
        out_shape=(jax.ShapeDtypeStruct((buf_rows, width) if carry_out else xd.shape, BF16), *grads),
        compiler_params=pltpu.CompilerParams(vmem_limit_bytes=63 * 1024 * 1024, dimension_semantics=('arbitrary',)),
        cost_estimate=pl.CostEstimate(flops=steps * n * (6 * rows * hidden + 8 * size * hidden), bytes_accessed=srcs * size * width * 4, transcendentals=0),
        name='run_experts',
    )(order, meta, xd, w, *extra)


def home_kernel(slot_ref, *refs):
    rets, (y_ref, dx_ref) = refs[:-2], refs[-2:]
    groups, size, width = rets[0].shape
    acc = None
    for c, ret in enumerate(rets):
        for g in range(groups):
            part = dot(pick_rows(slot_ref[g:g + 1, :], c * size, size), ret[g], 0, 0)
            acc = part if acc is None else acc + part
    y_ref[...] = acc[:, :width // 2].astype(BF16)
    dx_ref[...] = acc[:, width // 2:].astype(BF16)


def home_sum(slot, rets, block):
    groups, tokens = slot.shape
    _, size, width = rets[0].shape
    out = jax.ShapeDtypeStruct((tokens, width // 2), BF16)
    return pl.pallas_call(
        home_kernel,
        grid=(tokens // block,),
        out_shape=(out, out),
        in_specs=[pl.BlockSpec((groups, block), lambda i: (0, i))] + [pl.BlockSpec(memory_space=pltpu.VMEM)] * len(rets),
        out_specs=(pl.BlockSpec((block, width // 2), lambda i: (i, 0)),) * 2,
        compiler_params=pltpu.CompilerParams(vmem_limit_bytes=48 * 1024 * 1024),
        cost_estimate=pl.CostEstimate(flops=2 * groups * len(rets) * size * tokens * width, bytes_accessed=groups * size * width * 4, transcendentals=0),
        name='home_sum',
    )(slot, *rets)


def solution(mesh):
    groups = mesh.shape['grp']
    inner = mesh.shape['ing']
    tok_spec = P(('dp', 'grp', 'ing'), None)
    weight_spec = P(('grp', 'ing'), None, None)
    grad_spec = P(('dp', 'grp', 'ing'), None, None)
    chunks = 2

    def layer(x_loc, ids_loc, gates_loc, dy_loc, wg_loc, wu_loc, wd_loc):
        tokens, _ = x_loc.shape
        top_k = ids_loc.shape[1]
        per_group = wg_loc.shape[0] * inner
        group_limit = min(max(1, groups // 2), top_k // 2)
        cap = tokens * group_limit // groups
        swap = lambda a: lax.all_to_all(a, 'grp', 0, 0, tiled=True)
        w_own = jnp.concatenate([jnp.concatenate([wg_loc, wu_loc], axis=2), wd_loc], axis=1)
        w_all = lax.all_gather(w_own, 'ing', axis=0, tiled=True)
        size = cap // chunks
        slot, meta = make_tables(ids_loc.T, gates_loc.T, groups, per_group, cap, size)
        meta = swap(meta)
        recv = []
        for c in range(chunks):
            packed = pack_rows(slot, x_loc, dy_loc, c, size)
            if c == 0:
                packed, slot, meta = lax.optimization_barrier((packed, slot, meta))
            recv.append(swap(packed))
        me = lax.axis_index('ing')
        away = [inner // 2] + [i for i in range(1, inner) if i != inner // 2] + [0]
        order = (me + jnp.asarray(away, jnp.int32)) % inner
        everyone = list(range(per_group))
        ring = lambda a, d: lax.ppermute(a, 'ing', [(i, (i + d) % inner) for i in range(inner)])
        grads = None
        rets = []
        for c in range(chunks - 1):
            pq, grads = run_experts(c, order, everyone, meta, recv[c], w_all, grads)
            rets.append(swap(pq))
        c = chunks - 1
        ways = (1, -1, 1, -1)
        rows, *far = run_experts(c, order, everyone[:1], meta, recv[c], w_all, grads, None, True, True)
        for i, way in enumerate(ways):
            far[i] = ring(far[i], way)
        pq, *parts = run_experts(c, order, everyone[1:], meta, recv[c], w_all, grads, rows, False, True)
        after, before, own = parts[:4], parts[4:8], parts[8:]
        sums = [None] * 4
        for late in (False, True):
            for i, way in enumerate(ways):
                up, down = after[i], before[i]
                if late:
                    up, down = (up + far[i], None) if way == 1 else (None, down + far[i])
                else:
                    up, down = (None, down) if way == 1 else (up, None)
                sums[i] = (sums[i] or ()) + ((ring(up, 1),) if up is not None else (ring(down, -1),))
        rets.append(swap(pq))
        y_out, dx_out = home_sum(slot, rets, 256)
        g1, g3, g2a, g2b = [a + (b[0] + b[1]) for a, b in zip(own, sums)]
        return y_out, dx_out, g1[None], g3[None], jnp.concatenate([g2a, g2b], axis=0)[None]

    return jax.shard_map(layer, mesh=mesh, in_specs=(tok_spec, tok_spec, tok_spec, tok_spec, weight_spec, weight_spec, weight_spec), out_specs=(tok_spec, tok_spec, grad_spec, grad_spec, grad_spec), check_vma=False)
```

```python
import functools

import jax
import jax.numpy as jnp
from jax import lax
from jax.experimental import pallas as pl
from jax.experimental.pallas import tpu as pltpu
from jax.sharding import PartitionSpec as P


F32 = jnp.float32
BF16 = jnp.bfloat16
ALIGN = 16
TILE = 256


def dot(a, b, ca, cb):
    return lax.dot_general(a, b, (((ca,), (cb,)), ((), ())), preferred_element_type=F32)


def split3(v):
    hi = v.astype(BF16)
    rest = v - hi.astype(F32)
    mid = rest.astype(BF16)
    lo = (rest - mid.astype(F32)).astype(BF16)
    return jnp.concatenate([hi.astype(F32), mid.astype(F32), lo.astype(F32)], axis=0).astype(BF16)


def table_rows(groups, per_group, ids_ref, gates_ref, slots, vals):
    top_k, tokens = ids_ref.shape
    num_exp = groups * per_group
    exp_iota = lax.broadcasted_iota(jnp.int32, (num_exp, tokens), 0)
    grp_iota = lax.broadcasted_iota(jnp.int32, (groups, tokens), 0)
    mem = jnp.zeros((num_exp, tokens), F32)
    gate = jnp.zeros((num_exp, tokens), F32)
    gmem = jnp.zeros((groups, tokens), F32)
    for j in range(top_k):
        row = ids_ref[j:j + 1, :]
        hit = row == exp_iota
        mem = jnp.where(hit, 1.0, mem)
        gate = jnp.where(hit, gates_ref[j:j + 1, :], gate)
        gmem = jnp.where((row // per_group) == grp_iota, 1.0, gmem)
    upper = (lax.broadcasted_iota(jnp.int32, (tokens, tokens), 0) <= lax.broadcasted_iota(jnp.int32, (tokens, tokens), 1)).astype(F32).astype(BF16)
    rank = jnp.where(mem > 0, dot(mem.astype(BF16), upper, 1, 0), 0.0)
    slots[...] = jnp.where(gmem > 0, dot(gmem.astype(BF16), upper, 1, 0), 0.0)
    for g in range(groups):
        vals[g, 0:per_group, :] = rank[g * per_group:(g + 1) * per_group, :]
        vals[g, per_group:2 * per_group, :] = gate[g * per_group:(g + 1) * per_group, :]


def pick_rows(slot_row, first, count):
    want = (lax.broadcasted_iota(jnp.int32, (count, slot_row.shape[1]), 0) + (first + 1)).astype(F32)
    return (slot_row == want).astype(F32).astype(BF16)


def table_kernel(groups, per_group, size, ids_ref, gates_ref, slot_ref, meta_ref, vals):
    table_rows(groups, per_group, ids_ref, gates_ref, slot_ref, vals)
    n = 2 * per_group
    is_rank = lax.broadcasted_iota(jnp.int32, (n, 1), 0) < per_group

    @pl.loop(0, groups)
    def _(h):
        row = slot_ref[pl.ds(h, 1), :]
        split = split3(vals[h])
        base = jnp.zeros((n, 1), F32)
        for c in range(meta_ref.shape[2] // size):
            parts = dot(split, pick_rows(row, c * size, size), 1, 1)
            full = (parts[0:n] + parts[n:2 * n]) + parts[2 * n:3 * n]
            meta_ref[h, :, c * size:(c + 1) * size] = jnp.where(is_rank & (full > 0), full - base, full)
            base = jnp.where(is_rank, jnp.maximum(base, jnp.max(full, axis=1, keepdims=True)), 0.0)


def make_tables(ids_t, gates_t, groups, per_group, cap, size):
    tokens = ids_t.shape[1]
    vmem = pl.BlockSpec(memory_space=pltpu.VMEM)
    return pl.pallas_call(
        functools.partial(table_kernel, groups, per_group, size),
        out_shape=(jax.ShapeDtypeStruct((groups, tokens), F32), jax.ShapeDtypeStruct((groups, 2 * per_group, cap), F32)),
        in_specs=[vmem, vmem],
        out_specs=(vmem, vmem),
        scratch_shapes=[pltpu.VMEM((groups, 2 * per_group, tokens), F32)],
        cost_estimate=pl.CostEstimate(flops=2 * groups * cap * tokens * 128, bytes_accessed=groups * cap * 64, transcendentals=0),
        name='make_tables',
    )(ids_t, gates_t)


def pack_kernel(first, slot_ref, x_ref, dy_ref, packed_ref):
    size, width = packed_ref.shape[1:]
    pick = pick_rows(slot_ref[pl.ds(pl.program_id(0), 1), :], first, size)
    packed_ref[0, :, 0:width // 2] = dot(pick, x_ref[...], 1, 0).astype(BF16)
    packed_ref[0, :, width // 2:] = dot(pick, dy_ref[...], 1, 0).astype(BF16)


def pack_rows(slot, x, dy, c, size):
    groups, tokens = slot.shape
    hidden = x.shape[1]
    vmem = pl.BlockSpec(memory_space=pltpu.VMEM)
    return pl.pallas_call(
        functools.partial(pack_kernel, c * size),
        grid=(groups,),
        out_shape=jax.ShapeDtypeStruct((groups, size, 2 * hidden), BF16),
        in_specs=[vmem, vmem, vmem],
        out_specs=pl.BlockSpec((1, size, 2 * hidden), lambda h: (h, 0, 0)),
        compiler_params=pltpu.CompilerParams(vmem_limit_bytes=58 * 1024 * 1024),
        cost_estimate=pl.CostEstimate(flops=4 * groups * size * tokens * hidden, bytes_accessed=groups * size * hidden * 4, transcendentals=0),
        name='pack_rows',
    )(slot, x, dy)


def expert_kernel(chunk, first_pos, steps, has_prev, sums_in, sums_out, order_ref, meta_ref, xd_ref, w_ref, *refs):
    refs = list(refs)
    prev = refs.pop(0) if has_prev else None
    before = refs.pop(0) if sums_in else None
    rows_ref = refs.pop(0)
    split = sums_in or sums_out
    grad_refs = [refs.pop(0) for _ in range(2 * steps if split else 1)]
    buf, acc, pq, offs, in_sem, out_sem, sum_sem = refs[:7]
    stage, pq_sem = (None, None) if sums_out else refs[7:]
    step = pl.program_id(0)
    k = order_ref[first_pos + step]
    srcs, size, width = xd_ref.shape
    hidden = width // 2
    rows2 = meta_ref.shape[1]
    per_group = rows2 // 2
    ff = acc.shape[0] - hidden
    lanes = pl.ds(chunk * size, size)

    def each_grad(at, act):
        if not split:
            act(pltpu.make_async_copy(acc, grad_refs[0].at[at], out_sem.at[0]))
            return
        for i in range(steps):
            @pl.when(at == i)
            def _(i=i):
                for j in range(2):
                    act(pltpu.make_async_copy(acc.at[:, pl.ds(j * ff, ff)], grad_refs[2 * i + j], out_sem.at[j]))

    def load_prev():
        return pltpu.make_async_copy(prev.at[first_pos + step], acc, in_sem)

    @pl.when(step > 0)
    def _():
        each_grad(step - 1, lambda copy: copy.wait())

    if has_prev:
        load_prev().start()
    else:
        acc[...] = jnp.zeros_like(acc)

    if sums_in:
        @pl.when(step == 0)
        def _():
            pltpu.make_async_copy(before, pq, sum_sem).start()

    def pick(s):
        slot = (lax.broadcasted_iota(jnp.int32, (size, size), 0) + 1).astype(F32)
        return meta_ref[s, pl.ds(k, 1), lanes] == slot

    def gather(s, off):
        off = pl.multiple_of(off, ALIGN)
        offs[s] = off
        hit = pick(s)
        sel = hit.astype(F32).astype(BF16)
        gate = jnp.sum(jnp.where(hit, meta_ref[s, pl.ds(per_group + k, 1), lanes], 0.0), axis=1, keepdims=True)
        buf[pl.ds(off, size), 0:hidden] = dot(sel, xd_ref[s, :, 0:hidden], 1, 0).astype(BF16)
        buf[pl.ds(off, size), hidden:] = (gate * dot(sel, xd_ref[s, :, hidden:], 1, 0)).astype(BF16)
        count = jnp.max(meta_ref[s, pl.ds(k, 1), lanes]).astype(jnp.int32)
        return off + (count + ALIGN - 1) // ALIGN * ALIGN

    total = pl.multiple_of(lax.fori_loop(0, srcs, gather, jnp.int32(0)), ALIGN)
    buf[pl.ds(total, TILE), :] = jnp.zeros((TILE, width), BF16)
    if has_prev:
        load_prev().wait()

    @pl.loop(0, (total + TILE - 1) // TILE)
    def _(i):
        tile = pl.ds(pl.multiple_of(i * TILE, TILE), TILE)
        x = buf[tile, 0:hidden]
        d = buf[tile, hidden:]
        h = dot(x, w_ref[0, 0:hidden, :], 1, 0)
        da = dot(d, w_ref[0, hidden:, :], 1, 1)
        h1 = h[:, 0:ff]
        h3 = h[:, ff:]
        sig = jax.nn.sigmoid(h1)
        silu = h1 * sig
        a = (silu * h3).astype(BF16)
        dh1 = (da * h3 * sig * (1.0 + h1 * (1.0 - sig))).astype(BF16)
        dh3 = (da * silu).astype(BF16)
        dh = jnp.concatenate([dh1, dh3], axis=1)
        acc[0:hidden, :] += dot(x, dh, 0, 0)
        acc[hidden:, :] += dot(a, d, 0, 0)
        buf[tile, 0:hidden] = dot(a, w_ref[0, hidden:, :], 1, 0).astype(BF16)
        buf[tile, hidden:] = dot(dh, w_ref[0, 0:hidden, :], 1, 1).astype(BF16)

    each_grad(step, lambda copy: copy.start())
    if sums_in:
        @pl.when(step == 0)
        def _():
            pltpu.make_async_copy(before, pq, sum_sem).wait()

    def combine(first):
        @pl.loop(0, srcs)
        def _(s):
            off = pl.multiple_of(offs[s], ALIGN)
            sel = pick(s).astype(F32).astype(BF16)
            cols = jnp.transpose(meta_ref[s, :, lanes])
            lane = lax.broadcasted_iota(jnp.int32, (size, rows2), 1)
            gate = jnp.sum(jnp.where(lane == per_group + k, cols, 0.0), axis=1, keepdims=True)
            p = gate * dot(sel, buf[pl.ds(off, size), 0:hidden], 0, 0)
            q = dot(sel, buf[pl.ds(off, size), hidden:], 0, 0)
            if first:
                pq[s, :, 0:hidden] = p
                pq[s, :, hidden:] = q
            else:
                pq[s, :, 0:hidden] += p
                pq[s, :, hidden:] += q

    if sums_in or steps == 1:
        combine(not sums_in)
    else:
        @pl.when(step == 0)
        def _():
            combine(True)

        @pl.when(step > 0)
        def _():
            combine(False)

    @pl.when(step == steps - 1)
    def _():
        if sums_out:
            copy = pltpu.make_async_copy(pq, rows_ref, sum_sem)
            copy.start()
            copy.wait()
        else:
            for s in range(srcs):
                slot = s % 2
                if s >= 2:
                    pltpu.make_async_copy(stage.at[slot], rows_ref.at[s - 2], pq_sem.at[slot]).wait()
                stage[slot] = pq[s].astype(BF16)
                pltpu.make_async_copy(stage.at[slot], rows_ref.at[s], pq_sem.at[slot]).start()
            for s in range(max(0, srcs - 2), srcs):
                pltpu.make_async_copy(stage.at[s % 2], rows_ref.at[s], pq_sem.at[s % 2]).wait()
        each_grad(step, lambda copy: copy.wait())


def run_experts(chunk, order, positions, meta, xd, w, prev=None, sums=None, more=None):
    srcs, size, width = xd.shape
    _, rows, hidden = w.shape
    first, steps = positions[0], len(positions)
    any_spec = pl.BlockSpec(memory_space=pl.ANY)
    vmem = pl.BlockSpec(memory_space=pltpu.VMEM)
    extra = [a for a in (prev, sums) if a is not None]
    n = srcs * size // 2
    if more is None:
        grads = [jax.ShapeDtypeStruct((steps, rows, hidden), F32)]
    else:
        grads = [jax.ShapeDtypeStruct((rows, hidden // 2), F32)] * (2 * steps)
    scratch = [
        pltpu.VMEM((srcs * size + max(size, TILE), width), BF16),
        pltpu.VMEM((rows, hidden), F32),
        pltpu.VMEM((srcs, size, width), F32),
        pltpu.SMEM((srcs,), jnp.int32),
        pltpu.SemaphoreType.DMA,
        pltpu.SemaphoreType.DMA((2,)),
        pltpu.SemaphoreType.DMA,
    ]
    if not more:
        scratch += [pltpu.VMEM((2, size, width), BF16), pltpu.SemaphoreType.DMA((2,))]
    return pl.pallas_call(
        functools.partial(expert_kernel, chunk, first, steps, prev is not None, sums is not None, bool(more)),
        grid_spec=pltpu.PrefetchScalarGridSpec(
            num_scalar_prefetch=1,
            grid=(steps,),
            in_specs=[vmem, vmem, pl.BlockSpec((1, rows, hidden), lambda k, o: (o[first + k], 0, 0))] + [any_spec] * len(extra),
            out_specs=[any_spec] * (1 + len(grads)),
            scratch_shapes=scratch,
        ),
        out_shape=(jax.ShapeDtypeStruct(xd.shape, F32 if more else BF16), *grads),
        compiler_params=pltpu.CompilerParams(vmem_limit_bytes=63 * 1024 * 1024, dimension_semantics=('arbitrary',)),
        cost_estimate=pl.CostEstimate(flops=steps * n * (6 * rows * hidden + 8 * size * hidden), bytes_accessed=srcs * size * width * 4, transcendentals=0),
        name='run_experts',
    )(order, meta, xd, w, *extra)


def home_kernel(first, slot_ref, ret_ref, *refs):
    groups, size, width = ret_ref.shape
    acc = refs[0][...] if first else None
    outs = refs[1:] if first else refs
    for g in range(groups):
        part = dot(pick_rows(slot_ref[g:g + 1, :], first, size), ret_ref[g], 0, 0)
        acc = part if acc is None else acc + part
    if len(outs) == 1:
        outs[0][...] = acc
    else:
        outs[0][...] = acc[:, :width // 2].astype(BF16)
        outs[1][...] = acc[:, width // 2:].astype(BF16)


def home_sum(slot, ret, c, before, last, block):
    groups, tokens = slot.shape
    _, size, width = ret.shape
    rows = lambda w: pl.BlockSpec((block, w), lambda i: (i, 0))
    hidden = width // 2
    outs = [(hidden, BF16)] * 2 if last else [(width, F32)]
    extra = [] if before is None else [before]
    return pl.pallas_call(
        functools.partial(home_kernel, c * size),
        grid=(tokens // block,),
        out_shape=[jax.ShapeDtypeStruct((tokens, w), t) for w, t in outs],
        in_specs=[pl.BlockSpec((groups, block), lambda i: (0, i)), pl.BlockSpec(memory_space=pltpu.VMEM)] + [rows(width)] * len(extra),
        out_specs=[rows(w) for w, _ in outs],
        compiler_params=pltpu.CompilerParams(vmem_limit_bytes=48 * 1024 * 1024),
        cost_estimate=pl.CostEstimate(flops=2 * groups * size * tokens * width, bytes_accessed=groups * size * width * 2, transcendentals=0),
        name='home_sum',
    )(slot, ret, *extra)


def finish_kernel(*refs):
    g1_ref, g3_ref, g2_ref = refs[6:]
    tops = pl.num_programs(0) - pl.num_programs(0) // 3
    i = pl.program_id(0)
    left = refs[0][...] + (refs[1][...] + refs[2][...])
    right = refs[3][...] + (refs[4][...] + refs[5][...])

    @pl.when(i < tops)
    def _():
        g1_ref[0] = left
        g3_ref[0] = right

    @pl.when(i >= tops)
    def _():
        g2_ref[0] = jnp.concatenate([left, right], axis=1)


def finish(lefts, rights, hidden):
    rows, ff = lefts[0].shape
    assert rows == hidden + ff and hidden == 2 * ff
    block = ff // 2
    tops = hidden // block
    top = pl.BlockSpec((1, block, ff), lambda i: (0, jnp.minimum(i, tops - 1), 0))
    return pl.pallas_call(
        finish_kernel,
        grid=(rows // block,),
        out_shape=[jax.ShapeDtypeStruct((1,) + a, F32) for a in ((hidden, ff), (hidden, ff), (ff, hidden))],
        in_specs=[pl.BlockSpec((block, ff), lambda i: (i, 0))] * 6,
        out_specs=[top, top, pl.BlockSpec((1, block, hidden), lambda i: (0, jnp.maximum(i - tops, 0), 0))],
        compiler_params=pltpu.CompilerParams(vmem_limit_bytes=58 * 1024 * 1024),
        cost_estimate=pl.CostEstimate(flops=4 * rows * ff, bytes_accessed=32 * rows * ff, transcendentals=0),
        name='finish',
    )(*lefts, *rights)


def solution(mesh):
    groups = mesh.shape['grp']
    inner = mesh.shape['ing']
    tok_spec = P(('dp', 'grp', 'ing'), None)
    weight_spec = P(('grp', 'ing'), None, None)
    grad_spec = P(('dp', 'grp', 'ing'), None, None)
    chunks = 2

    def layer(x_loc, ids_loc, gates_loc, dy_loc, wg_loc, wu_loc, wd_loc):
        tokens, hidden = x_loc.shape
        top_k = ids_loc.shape[1]
        per_group = wg_loc.shape[0] * inner
        group_limit = min(max(1, groups // 2), top_k // 2)
        cap = tokens * group_limit // groups
        swap = lambda a: lax.all_to_all(a, 'grp', 0, 0, tiled=True)
        w_own = jnp.concatenate([jnp.concatenate([wg_loc, wu_loc], axis=2), wd_loc], axis=1)
        w_all = lax.all_gather(w_own, 'ing', axis=0, tiled=True)
        size = cap // chunks
        slot, meta = make_tables(ids_loc.T, gates_loc.T, groups, per_group, cap, size)
        meta = swap(meta)
        recv = []
        for c in range(chunks):
            packed = pack_rows(slot, x_loc, dy_loc, c, size)
            if c == 0:
                packed, slot, meta = lax.optimization_barrier((packed, slot, meta))
            recv.append(swap(packed))
        me = lax.axis_index('ing')
        away = [inner // 2] + [i for i in range(1, inner) if i != inner // 2] + [0]
        order = (me + jnp.asarray(away, jnp.int32)) % inner
        everyone = list(range(per_group))
        ring = lambda a, d: lax.ppermute(a, 'ing', [(i, (i + d) % inner) for i in range(inner)])
        grads = None
        total = None
        c = chunks - 1
        rets = []
        for i in range(c):
            pq, grads = run_experts(i, order, everyone, meta, recv[i], w_all, grads)
            rets.append(swap(pq))
        sums, *far = run_experts(c, order, everyone[:1], meta, recv[c], w_all, grads, None, True)
        far0 = ring(far[0], 1)
        far1 = ring(far[1], -1)
        sums, next0, next1, last0, last1 = run_experts(c, order, everyone[1:-1], meta, recv[c], w_all, grads, sums, True)
        soon1 = ring(next1, 1)
        soon0 = ring(last0, -1)
        pq, own0, own1 = run_experts(c, order, everyone[-1:], meta, recv[c], w_all, grads, sums, False)
        rets.append(swap(pq))
        late0 = ring(next0 + far0, 1)
        late1 = ring(last1 + far1, -1)
        for i in range(chunks):
            total = home_sum(slot, rets[i], i, total, i == c, 256)
            total = total[0] if i < c else total
        y_out, dx_out = total
        g1, g3, g2 = finish((own0, soon0, late0), (own1, soon1, late1), hidden)
        return y_out, dx_out, g1, g3, g2

    return jax.shard_map(layer, mesh=mesh, in_specs=(tok_spec, tok_spec, tok_spec, tok_spec, weight_spec, weight_spec, weight_spec), out_specs=(tok_spec, tok_spec, grad_spec, grad_spec, grad_spec), check_vma=False)
```

```python
import functools

import jax
import jax.numpy as jnp
from jax import lax
from jax.experimental import pallas as pl
from jax.experimental.pallas import tpu as pltpu
from jax.sharding import PartitionSpec as P


F32 = jnp.float32
BF16 = jnp.bfloat16
ALIGN = 16
TILE = 256


def dot(a, b, ca, cb):
    return lax.dot_general(a, b, (((ca,), (cb,)), ((), ())), preferred_element_type=F32)


def split3(v):
    hi = v.astype(BF16)
    rest = v - hi.astype(F32)
    mid = rest.astype(BF16)
    lo = (rest - mid.astype(F32)).astype(BF16)
    return jnp.concatenate([hi.astype(F32), mid.astype(F32), lo.astype(F32)], axis=0).astype(BF16)


def table_rows(groups, per_group, ids_ref, gates_ref, slots, vals):
    top_k, tokens = ids_ref.shape
    num_exp = groups * per_group
    exp_iota = lax.broadcasted_iota(jnp.int32, (num_exp, tokens), 0)
    grp_iota = lax.broadcasted_iota(jnp.int32, (groups, tokens), 0)
    mem = jnp.zeros((num_exp, tokens), F32)
    gate = jnp.zeros((num_exp, tokens), F32)
    gmem = jnp.zeros((groups, tokens), F32)
    for j in range(top_k):
        row = ids_ref[j:j + 1, :]
        hit = row == exp_iota
        mem = jnp.where(hit, 1.0, mem)
        gate = jnp.where(hit, gates_ref[j:j + 1, :], gate)
        gmem = jnp.where((row // per_group) == grp_iota, 1.0, gmem)
    upper = (lax.broadcasted_iota(jnp.int32, (tokens, tokens), 0) <= lax.broadcasted_iota(jnp.int32, (tokens, tokens), 1)).astype(F32).astype(BF16)
    rank = jnp.where(mem > 0, dot(mem.astype(BF16), upper, 1, 0), 0.0)
    slots[...] = jnp.where(gmem > 0, dot(gmem.astype(BF16), upper, 1, 0), 0.0)
    for g in range(groups):
        vals[g, 0:per_group, :] = rank[g * per_group:(g + 1) * per_group, :]
        vals[g, per_group:2 * per_group, :] = gate[g * per_group:(g + 1) * per_group, :]


def pick_rows(slot_row, first, count):
    want = (lax.broadcasted_iota(jnp.int32, (count, slot_row.shape[1]), 0) + (first + 1)).astype(F32)
    return (slot_row == want).astype(F32).astype(BF16)


def table_kernel(groups, per_group, size, ids_ref, gates_ref, *refs):
    weights, (slot_ref, meta_ref, joined_ref, vals, joined, sems) = refs[:3], refs[3:]
    hidden, ff = weights[0].shape[1:]
    places = ((pl.ds(0, hidden), pl.ds(0, ff)), (pl.ds(0, hidden), pl.ds(ff, ff)), (pl.ds(hidden, ff), pl.ds(0, hidden)))
    loads = [pltpu.make_async_copy(weights[i].at[0], joined.at[r, c], sems.at[i]) for i, (r, c) in enumerate(places)]
    store = pltpu.make_async_copy(joined, joined_ref.at[0], sems.at[3])
    for copy in loads:
        copy.start()
    table_rows(groups, per_group, ids_ref, gates_ref, slot_ref, vals)
    for copy in loads:
        copy.wait()
    store.start()
    n = 2 * per_group
    is_rank = lax.broadcasted_iota(jnp.int32, (n, 1), 0) < per_group

    @pl.loop(0, groups)
    def _(h):
        row = slot_ref[pl.ds(h, 1), :]
        split = split3(vals[h])
        base = jnp.zeros((n, 1), F32)
        for c in range(meta_ref.shape[2] // size):
            parts = dot(split, pick_rows(row, c * size, size), 1, 1)
            full = (parts[0:n] + parts[n:2 * n]) + parts[2 * n:3 * n]
            meta_ref[h, :, c * size:(c + 1) * size] = jnp.where(is_rank & (full > 0), full - base, full)
            base = jnp.where(is_rank, jnp.maximum(base, jnp.max(full, axis=1, keepdims=True)), 0.0)

    store.wait()


def make_tables(ids_t, gates_t, weights, groups, per_group, cap, size):
    tokens = ids_t.shape[1]
    vmem = pl.BlockSpec(memory_space=pltpu.VMEM)
    any_spec = pl.BlockSpec(memory_space=pl.ANY)
    _, hidden, ff = weights[0].shape
    assert hidden == 2 * ff and weights[2].shape == (1, ff, hidden)
    joined = (hidden + ff, hidden)
    return pl.pallas_call(
        functools.partial(table_kernel, groups, per_group, size),
        out_shape=(
            jax.ShapeDtypeStruct((groups, tokens), F32),
            jax.ShapeDtypeStruct((groups, 2 * per_group, cap), F32),
            jax.ShapeDtypeStruct((1,) + joined, BF16),
        ),
        in_specs=[vmem, vmem] + [any_spec] * 3,
        out_specs=(vmem, vmem, any_spec),
        scratch_shapes=[
            pltpu.VMEM((groups, 2 * per_group, tokens), F32),
            pltpu.VMEM(joined, BF16),
            pltpu.SemaphoreType.DMA((4,)),
        ],
        compiler_params=pltpu.CompilerParams(vmem_limit_bytes=58 * 1024 * 1024),
        cost_estimate=pl.CostEstimate(flops=2 * groups * cap * tokens * 128, bytes_accessed=groups * cap * 64, transcendentals=0),
        name='make_tables',
    )(ids_t, gates_t, *weights)


def pack_kernel(first, slot_ref, x_ref, dy_ref, packed_ref):
    size, width = packed_ref.shape[1:]
    pick = pick_rows(slot_ref[pl.ds(pl.program_id(0), 1), :], first, size)
    packed_ref[0, :, 0:width // 2] = dot(pick, x_ref[...], 1, 0).astype(BF16)
    packed_ref[0, :, width // 2:] = dot(pick, dy_ref[...], 1, 0).astype(BF16)


def pack_rows(slot, x, dy, c, size):
    groups, tokens = slot.shape
    hidden = x.shape[1]
    vmem = pl.BlockSpec(memory_space=pltpu.VMEM)
    return pl.pallas_call(
        functools.partial(pack_kernel, c * size),
        grid=(groups,),
        out_shape=jax.ShapeDtypeStruct((groups, size, 2 * hidden), BF16),
        in_specs=[vmem, vmem, vmem],
        out_specs=pl.BlockSpec((1, size, 2 * hidden), lambda h: (h, 0, 0)),
        compiler_params=pltpu.CompilerParams(vmem_limit_bytes=58 * 1024 * 1024),
        cost_estimate=pl.CostEstimate(flops=4 * groups * size * tokens * hidden, bytes_accessed=groups * size * hidden * 4, transcendentals=0),
        name='pack_rows',
    )(slot, x, dy)


def expert_kernel(chunk, first_pos, steps, has_prev, sums_in, sums_out, order_ref, meta_ref, xd_ref, w_ref, *refs):
    refs = list(refs)
    prev = refs.pop(0) if has_prev else None
    before = refs.pop(0) if sums_in else None
    rows_ref = refs.pop(0)
    split = sums_in or sums_out
    grad_refs = [refs.pop(0) for _ in range(2 * steps if split else 1)]
    buf, acc, pq, xd, w, offs, in_sem, out_sem, sum_sem, xd_sem, w_sem = refs[:11]
    stage, pq_sem = (None, None) if sums_out else refs[11:]
    step = pl.program_id(0)
    k = order_ref[first_pos + step]
    srcs, size, width = xd_ref.shape
    hidden = width // 2
    rows2 = meta_ref.shape[1]
    per_group = rows2 // 2
    ff = acc.shape[0] - hidden
    lanes = pl.ds(chunk * size, size)

    def each_grad(at, act):
        if not split:
            act(pltpu.make_async_copy(acc, grad_refs[0].at[at], out_sem.at[0]))
            return
        for i in range(steps):
            @pl.when(at == i)
            def _(i=i):
                for j in range(2):
                    act(pltpu.make_async_copy(acc.at[:, pl.ds(j * ff, ff)], grad_refs[2 * i + j], out_sem.at[j]))

    def load_prev():
        return pltpu.make_async_copy(prev.at[first_pos + step], acc, in_sem)

    def load_rows(s):
        return pltpu.make_async_copy(xd_ref.at[s], xd.at[s], xd_sem.at[s])

    def load_weights(at):
        slot = at % 2
        return pltpu.make_async_copy(w_ref.at[order_ref[first_pos + at]], w.at[slot], w_sem.at[slot])

    @pl.when(step == 0)
    def _():
        @pl.loop(0, srcs)
        def _(s):
            load_rows(s).start()

        load_weights(0).start()

    if steps > 1:
        @pl.when(step < steps - 1)
        def _():
            load_weights(step + 1).start()

    @pl.when(step > 0)
    def _():
        each_grad(step - 1, lambda copy: copy.wait())

    if has_prev:
        load_prev().start()
    else:
        acc[...] = jnp.zeros_like(acc)

    if sums_in:
        @pl.when(step == 0)
        def _():
            pltpu.make_async_copy(before, pq, sum_sem).start()

    def pick(s):
        slot = (lax.broadcasted_iota(jnp.int32, (size, size), 0) + 1).astype(F32)
        return meta_ref[s, pl.ds(k, 1), lanes] == slot

    def gather(s, off):
        @pl.when(step == 0)
        def _():
            load_rows(s).wait()

        off = pl.multiple_of(off, ALIGN)
        offs[s] = off
        hit = pick(s)
        sel = hit.astype(F32).astype(BF16)
        gate = jnp.sum(jnp.where(hit, meta_ref[s, pl.ds(per_group + k, 1), lanes], 0.0), axis=1, keepdims=True)
        buf[pl.ds(off, size), 0:hidden] = dot(sel, xd[s, :, 0:hidden], 1, 0).astype(BF16)
        buf[pl.ds(off, size), hidden:] = (gate * dot(sel, xd[s, :, hidden:], 1, 0)).astype(BF16)
        count = jnp.max(meta_ref[s, pl.ds(k, 1), lanes]).astype(jnp.int32)
        return off + (count + ALIGN - 1) // ALIGN * ALIGN

    total = pl.multiple_of(lax.fori_loop(0, srcs, gather, jnp.int32(0)), ALIGN)
    buf[pl.ds(total, TILE), :] = jnp.zeros((TILE, width), BF16)
    if has_prev:
        load_prev().wait()
    load_weights(step).wait()
    ws = step % 2

    @pl.loop(0, (total + TILE - 1) // TILE)
    def _(i):
        tile = pl.ds(pl.multiple_of(i * TILE, TILE), TILE)
        x = buf[tile, 0:hidden]
        d = buf[tile, hidden:]
        h = dot(x, w[ws, 0:hidden, :], 1, 0)
        da = dot(d, w[ws, hidden:, :], 1, 1)
        h1 = h[:, 0:ff]
        h3 = h[:, ff:]
        sig = jax.nn.sigmoid(h1)
        silu = h1 * sig
        a = (silu * h3).astype(BF16)
        dh1 = (da * h3 * sig * (1.0 + h1 * (1.0 - sig))).astype(BF16)
        dh3 = (da * silu).astype(BF16)
        dh = jnp.concatenate([dh1, dh3], axis=1)
        acc[0:hidden, :] += dot(x, dh, 0, 0)
        acc[hidden:, :] += dot(a, d, 0, 0)
        buf[tile, 0:hidden] = dot(a, w[ws, hidden:, :], 1, 0).astype(BF16)
        buf[tile, hidden:] = dot(dh, w[ws, 0:hidden, :], 1, 1).astype(BF16)

    each_grad(step, lambda copy: copy.start())
    if sums_in:
        @pl.when(step == 0)
        def _():
            pltpu.make_async_copy(before, pq, sum_sem).wait()

    def combine(first, last):
        @pl.loop(0, srcs)
        def _(s):
            off = pl.multiple_of(offs[s], ALIGN)
            sel = pick(s).astype(F32).astype(BF16)
            cols = jnp.transpose(meta_ref[s, :, lanes])
            lane = lax.broadcasted_iota(jnp.int32, (size, rows2), 1)
            gate = jnp.sum(jnp.where(lane == per_group + k, cols, 0.0), axis=1, keepdims=True)
            p = gate * dot(sel, buf[pl.ds(off, size), 0:hidden], 0, 0)
            q = dot(sel, buf[pl.ds(off, size), hidden:], 0, 0)
            if not first:
                p = pq[s, :, 0:hidden] + p
                q = pq[s, :, hidden:] + q
            if last and not sums_out:
                slot = s % 2

                @pl.when(s >= 2)
                def _():
                    pltpu.make_async_copy(stage.at[slot], rows_ref.at[s - 2], pq_sem.at[slot]).wait()

                stage[slot, :, 0:hidden] = p.astype(BF16)
                stage[slot, :, hidden:] = q.astype(BF16)
                pltpu.make_async_copy(stage.at[slot], rows_ref.at[s], pq_sem.at[slot]).start()
                return
            pq[s, :, 0:hidden] = p
            pq[s, :, hidden:] = q
            if last:
                pltpu.make_async_copy(pq.at[s], rows_ref.at[s], pq_out.at[s]).start()

    pq_out = xd_sem
    if steps == 1:
        combine(not sums_in, True)
    else:
        if not sums_in:
            @pl.when(step == 0)
            def _():
                combine(True, False)

        if sums_in or steps > 2:
            @pl.when((step < steps - 1) if sums_in else ((step > 0) & (step < steps - 1)))
            def _():
                combine(False, False)

        @pl.when(step == steps - 1)
        def _():
            combine(False, True)

    @pl.when(step == steps - 1)
    def _():
        if sums_out:
            for s in range(srcs):
                pltpu.make_async_copy(pq.at[s], rows_ref.at[s], pq_out.at[s]).wait()
        else:
            for s in range(max(0, srcs - 2), srcs):
                pltpu.make_async_copy(stage.at[s % 2], rows_ref.at[s], pq_sem.at[s % 2]).wait()
        each_grad(step, lambda copy: copy.wait())


def run_experts(chunk, order, positions, meta, xd, w, prev=None, sums=None, more=None):
    srcs, size, width = xd.shape
    _, rows, hidden = w.shape
    first, steps = positions[0], len(positions)
    any_spec = pl.BlockSpec(memory_space=pl.ANY)
    vmem = pl.BlockSpec(memory_space=pltpu.VMEM)
    extra = [a for a in (prev, sums) if a is not None]
    n = srcs * size // 2
    if more is None:
        grads = [jax.ShapeDtypeStruct((steps, rows, hidden), F32)]
    else:
        grads = [jax.ShapeDtypeStruct((rows, hidden // 2), F32)] * (2 * steps)
    scratch = [
        pltpu.VMEM((srcs * size + max(size, TILE), width), BF16),
        pltpu.VMEM((rows, hidden), F32),
        pltpu.VMEM((srcs, size, width), F32),
        pltpu.VMEM((srcs, size, width), BF16),
        pltpu.VMEM((2, rows, hidden), BF16),
        pltpu.SMEM((srcs,), jnp.int32),
        pltpu.SemaphoreType.DMA,
        pltpu.SemaphoreType.DMA((2,)),
        pltpu.SemaphoreType.DMA,
        pltpu.SemaphoreType.DMA((srcs,)),
        pltpu.SemaphoreType.DMA((2,)),
    ]
    if not more:
        scratch += [pltpu.VMEM((2, size, width), BF16), pltpu.SemaphoreType.DMA((2,))]
    return pl.pallas_call(
        functools.partial(expert_kernel, chunk, first, steps, prev is not None, sums is not None, bool(more)),
        grid_spec=pltpu.PrefetchScalarGridSpec(
            num_scalar_prefetch=1,
            grid=(steps,),
            in_specs=[vmem, any_spec, any_spec] + [any_spec] * len(extra),
            out_specs=[any_spec] * (1 + len(grads)),
            scratch_shapes=scratch,
        ),
        out_shape=(jax.ShapeDtypeStruct(xd.shape, F32 if more else BF16), *grads),
        compiler_params=pltpu.CompilerParams(vmem_limit_bytes=63 * 1024 * 1024, dimension_semantics=('arbitrary',)),
        cost_estimate=pl.CostEstimate(flops=steps * n * (6 * rows * hidden + 8 * size * hidden), bytes_accessed=srcs * size * width * 4, transcendentals=0),
        name='run_experts',
    )(order, meta, xd, w, *extra)


def home_kernel(first, slot_ref, ret_ref, *refs):
    groups, size, width = ret_ref.shape
    acc = refs[0][...] if first else None
    outs = refs[1:] if first else refs
    for g in range(groups):
        part = dot(pick_rows(slot_ref[g:g + 1, :], first, size), ret_ref[g], 0, 0)
        acc = part if acc is None else acc + part
    if len(outs) == 1:
        outs[0][...] = acc
    else:
        outs[0][...] = acc[:, :width // 2].astype(BF16)
        outs[1][...] = acc[:, width // 2:].astype(BF16)


def home_sum(slot, ret, c, before, last, block):
    groups, tokens = slot.shape
    _, size, width = ret.shape
    rows = lambda w: pl.BlockSpec((block, w), lambda i: (i, 0))
    hidden = width // 2
    outs = [(hidden, BF16)] * 2 if last else [(width, F32)]
    extra = [] if before is None else [before]
    return pl.pallas_call(
        functools.partial(home_kernel, c * size),
        grid=(tokens // block,),
        out_shape=[jax.ShapeDtypeStruct((tokens, w), t) for w, t in outs],
        in_specs=[pl.BlockSpec((groups, block), lambda i: (0, i)), pl.BlockSpec(memory_space=pltpu.VMEM)] + [rows(width)] * len(extra),
        out_specs=[rows(w) for w, _ in outs],
        compiler_params=pltpu.CompilerParams(vmem_limit_bytes=48 * 1024 * 1024),
        cost_estimate=pl.CostEstimate(flops=2 * groups * size * tokens * width, bytes_accessed=groups * size * width * 2, transcendentals=0),
        name='home_sum',
    )(slot, ret, *extra)


def finish_kernel(*refs):
    g1_ref, g3_ref, g2_ref = refs[6:]
    tops = pl.num_programs(0) - pl.num_programs(0) // 3
    i = pl.program_id(0)
    left = refs[0][...] + (refs[1][...] + refs[2][...])
    right = refs[3][...] + (refs[4][...] + refs[5][...])

    @pl.when(i < tops)
    def _():
        g1_ref[0] = left
        g3_ref[0] = right

    @pl.when(i >= tops)
    def _():
        g2_ref[0] = jnp.concatenate([left, right], axis=1)


def finish(lefts, rights, hidden):
    rows, ff = lefts[0].shape
    assert rows == hidden + ff and hidden == 2 * ff
    block = ff // 2
    tops = hidden // block
    top = pl.BlockSpec((1, block, ff), lambda i: (0, jnp.minimum(i, tops - 1), 0))
    return pl.pallas_call(
        finish_kernel,
        grid=(rows // block,),
        out_shape=[jax.ShapeDtypeStruct((1,) + a, F32) for a in ((hidden, ff), (hidden, ff), (ff, hidden))],
        in_specs=[pl.BlockSpec((block, ff), lambda i: (i, 0))] * 6,
        out_specs=[top, top, pl.BlockSpec((1, block, hidden), lambda i: (0, jnp.maximum(i - tops, 0), 0))],
        compiler_params=pltpu.CompilerParams(vmem_limit_bytes=58 * 1024 * 1024),
        cost_estimate=pl.CostEstimate(flops=4 * rows * ff, bytes_accessed=32 * rows * ff, transcendentals=0),
        name='finish',
    )(*lefts, *rights)


def solution(mesh):
    groups = mesh.shape['grp']
    inner = mesh.shape['ing']
    tok_spec = P(('dp', 'grp', 'ing'), None)
    weight_spec = P(('grp', 'ing'), None, None)
    grad_spec = P(('dp', 'grp', 'ing'), None, None)
    chunks = 2

    def layer(x_loc, ids_loc, gates_loc, dy_loc, wg_loc, wu_loc, wd_loc):
        tokens, hidden = x_loc.shape
        top_k = ids_loc.shape[1]
        per_group = wg_loc.shape[0] * inner
        group_limit = min(max(1, groups // 2), top_k // 2)
        cap = tokens * group_limit // groups
        swap = lambda a: lax.all_to_all(a, 'grp', 0, 0, tiled=True)
        size = cap // chunks
        slot, meta, w_own = make_tables(ids_loc.T, gates_loc.T, (wg_loc, wu_loc, wd_loc), groups, per_group, cap, size)
        w_all = lax.all_gather(w_own, 'ing', axis=0, tiled=True)
        meta = swap(meta)
        recv = []
        for c in range(chunks):
            packed = pack_rows(slot, x_loc, dy_loc, c, size)
            if c == 0:
                packed, slot, meta = lax.optimization_barrier((packed, slot, meta))
            recv.append(swap(packed))
        me = lax.axis_index('ing')
        away = [inner // 2] + [i for i in range(1, inner) if i != inner // 2] + [0]
        order = (me + jnp.asarray(away, jnp.int32)) % inner
        everyone = list(range(per_group))
        ring = lambda a, d: lax.ppermute(a, 'ing', [(i, (i + d) % inner) for i in range(inner)])
        grads = None
        total = None
        c = chunks - 1
        rets = []
        for i in range(c):
            pq, grads = run_experts(i, order, everyone, meta, recv[i], w_all, grads)
            rets.append(swap(pq))
        sums, *far = run_experts(c, order, everyone[:1], meta, recv[c], w_all, grads, None, True)
        far0 = ring(far[0], 1)
        far1 = ring(far[1], -1)
        sums, next0, next1, last0, last1 = run_experts(c, order, everyone[1:-1], meta, recv[c], w_all, grads, sums, True)
        soon1 = ring(next1, 1)
        soon0 = ring(last0, -1)
        pq, own0, own1 = run_experts(c, order, everyone[-1:], meta, recv[c], w_all, grads, sums, False)
        rets.append(swap(pq))
        late0 = ring(next0 + far0, 1)
        late1 = ring(last1 + far1, -1)
        for i in range(chunks):
            total = home_sum(slot, rets[i], i, total, i == c, 256)
            total = total[0] if i < c else total
        y_out, dx_out = total
        g1, g3, g2 = finish((own0, soon0, late0), (own1, soon1, late1), hidden)
        return y_out, dx_out, g1, g3, g2

    return jax.shard_map(layer, mesh=mesh, in_specs=(tok_spec, tok_spec, tok_spec, tok_spec, weight_spec, weight_spec, weight_spec), out_specs=(tok_spec, tok_spec, grad_spec, grad_spec, grad_spec), check_vma=False)
```

```python
import functools

import jax
import jax.numpy as jnp
from jax import lax
from jax.experimental import pallas as pl
from jax.experimental.pallas import tpu as pltpu
from jax.sharding import PartitionSpec as P


F32 = jnp.float32
BF16 = jnp.bfloat16
ALIGN = 16
TILE = 256


def dot(a, b, ca, cb):
    return lax.dot_general(a, b, (((ca,), (cb,)), ((), ())), preferred_element_type=F32)


def split3(v):
    hi = v.astype(BF16)
    rest = v - hi.astype(F32)
    mid = rest.astype(BF16)
    lo = (rest - mid.astype(F32)).astype(BF16)
    return jnp.concatenate([hi.astype(F32), mid.astype(F32), lo.astype(F32)], axis=0).astype(BF16)


def table_rows(groups, per_group, ids_ref, gates_ref, slots, vals):
    top_k, tokens = ids_ref.shape
    num_exp = groups * per_group
    exp_iota = lax.broadcasted_iota(jnp.int32, (num_exp, tokens), 0)
    grp_iota = lax.broadcasted_iota(jnp.int32, (groups, tokens), 0)
    mem = jnp.zeros((num_exp, tokens), F32)
    gate = jnp.zeros((num_exp, tokens), F32)
    gmem = jnp.zeros((groups, tokens), F32)
    for j in range(top_k):
        row = ids_ref[j:j + 1, :]
        hit = row == exp_iota
        mem = jnp.where(hit, 1.0, mem)
        gate = jnp.where(hit, gates_ref[j:j + 1, :], gate)
        gmem = jnp.where((row // per_group) == grp_iota, 1.0, gmem)
    upper = (lax.broadcasted_iota(jnp.int32, (tokens, tokens), 0) <= lax.broadcasted_iota(jnp.int32, (tokens, tokens), 1)).astype(F32).astype(BF16)
    rank = jnp.where(mem > 0, dot(mem.astype(BF16), upper, 1, 0), 0.0)
    slots[...] = jnp.where(gmem > 0, dot(gmem.astype(BF16), upper, 1, 0), 0.0)
    for g in range(groups):
        vals[g, 0:per_group, :] = rank[g * per_group:(g + 1) * per_group, :]
        vals[g, per_group:2 * per_group, :] = gate[g * per_group:(g + 1) * per_group, :]


def pick_rows(slot_row, first, count):
    want = (lax.broadcasted_iota(jnp.int32, (count, slot_row.shape[1]), 0) + (first + 1)).astype(F32)
    return (slot_row == want).astype(F32).astype(BF16)


def table_kernel(groups, per_group, size, ids_ref, gates_ref, *refs):
    weights, (slot_ref, meta_ref, joined_ref, vals, joined, sems) = refs[:3], refs[3:]
    hidden, ff = weights[0].shape[1:]
    places = ((pl.ds(0, hidden), pl.ds(0, ff)), (pl.ds(0, hidden), pl.ds(ff, ff)), (pl.ds(hidden, ff), pl.ds(0, hidden)))
    loads = [pltpu.make_async_copy(weights[i].at[0], joined.at[r, c], sems.at[i]) for i, (r, c) in enumerate(places)]
    store = pltpu.make_async_copy(joined, joined_ref.at[0], sems.at[3])
    for copy in loads:
        copy.start()
    table_rows(groups, per_group, ids_ref, gates_ref, slot_ref, vals)
    for copy in loads:
        copy.wait()
    store.start()
    n = 2 * per_group
    is_rank = lax.broadcasted_iota(jnp.int32, (n, 1), 0) < per_group

    @pl.loop(0, groups)
    def _(h):
        row = slot_ref[pl.ds(h, 1), :]
        split = split3(vals[h])
        base = jnp.zeros((n, 1), F32)
        for c in range(meta_ref.shape[2] // size):
            parts = dot(split, pick_rows(row, c * size, size), 1, 1)
            full = (parts[0:n] + parts[n:2 * n]) + parts[2 * n:3 * n]
            meta_ref[h, :, c * size:(c + 1) * size] = jnp.where(is_rank & (full > 0), full - base, full)
            base = jnp.where(is_rank, jnp.maximum(base, jnp.max(full, axis=1, keepdims=True)), 0.0)

    store.wait()


def make_tables(ids_t, gates_t, weights, groups, per_group, cap, size):
    tokens = ids_t.shape[1]
    vmem = pl.BlockSpec(memory_space=pltpu.VMEM)
    any_spec = pl.BlockSpec(memory_space=pl.ANY)
    _, hidden, ff = weights[0].shape
    assert hidden == 2 * ff and weights[2].shape == (1, ff, hidden)
    joined = (hidden + ff, hidden)
    return pl.pallas_call(
        functools.partial(table_kernel, groups, per_group, size),
        out_shape=(
            jax.ShapeDtypeStruct((groups, tokens), F32),
            jax.ShapeDtypeStruct((groups, 2 * per_group, cap), F32),
            jax.ShapeDtypeStruct((1,) + joined, BF16),
        ),
        in_specs=[vmem, vmem] + [any_spec] * 3,
        out_specs=(vmem, vmem, any_spec),
        scratch_shapes=[
            pltpu.VMEM((groups, 2 * per_group, tokens), F32),
            pltpu.VMEM(joined, BF16),
            pltpu.SemaphoreType.DMA((4,)),
        ],
        compiler_params=pltpu.CompilerParams(vmem_limit_bytes=58 * 1024 * 1024),
        cost_estimate=pl.CostEstimate(flops=2 * groups * cap * tokens * 128, bytes_accessed=groups * cap * 64, transcendentals=0),
        name='make_tables',
    )(ids_t, gates_t, *weights)


def pack_kernel(first, slot_ref, x_ref, dy_ref, packed_ref):
    size, width = packed_ref.shape[1:]
    pick = pick_rows(slot_ref[pl.ds(pl.program_id(0), 1), :], first, size)
    packed_ref[0, :, 0:width // 2] = dot(pick, x_ref[...], 1, 0).astype(BF16)
    packed_ref[0, :, width // 2:] = dot(pick, dy_ref[...], 1, 0).astype(BF16)


def pack_rows(slot, x, dy, c, size):
    groups, tokens = slot.shape
    hidden = x.shape[1]
    vmem = pl.BlockSpec(memory_space=pltpu.VMEM)
    return pl.pallas_call(
        functools.partial(pack_kernel, c * size),
        grid=(groups,),
        out_shape=jax.ShapeDtypeStruct((groups, size, 2 * hidden), BF16),
        in_specs=[vmem, vmem, vmem],
        out_specs=pl.BlockSpec((1, size, 2 * hidden), lambda h: (h, 0, 0)),
        compiler_params=pltpu.CompilerParams(vmem_limit_bytes=58 * 1024 * 1024),
        cost_estimate=pl.CostEstimate(flops=4 * groups * size * tokens * hidden, bytes_accessed=groups * size * hidden * 4, transcendentals=0),
        name='pack_rows',
    )(slot, x, dy)


def expert_kernel(chunk, first_pos, steps, has_prev, sums_in, sums_out, order_ref, meta_ref, xd_ref, w_ref, *refs):
    refs = list(refs)
    prev = refs.pop(0) if has_prev else None
    before = refs.pop(0) if sums_in else None
    rows_ref = refs.pop(0)
    split = sums_in or sums_out
    grad_refs = [refs.pop(0) for _ in range(2 * steps if split else 1)]
    buf, acc, pq, xd, w, offs, in_sem, out_sem, sum_sem, xd_sem, w_sem = refs[:11]
    stage, pq_sem = (None, None) if sums_out else refs[11:]
    step = pl.program_id(0)
    k = order_ref[first_pos + step]
    srcs, size, width = xd_ref.shape
    hidden = width // 2
    rows2 = meta_ref.shape[1]
    per_group = rows2 // 2
    ff = acc.shape[0] - hidden
    lanes = pl.ds(chunk * size, size)

    def each_grad(at, act):
        if not split:
            act(pltpu.make_async_copy(acc, grad_refs[0].at[at], out_sem.at[0]))
            return
        for i in range(steps):
            @pl.when(at == i)
            def _(i=i):
                for j in range(2):
                    act(pltpu.make_async_copy(acc.at[:, pl.ds(j * ff, ff)], grad_refs[2 * i + j], out_sem.at[j]))

    def load_prev():
        return pltpu.make_async_copy(prev.at[first_pos + step], acc, in_sem)

    def load_rows(s):
        return pltpu.make_async_copy(xd_ref.at[s], xd.at[s], xd_sem.at[s])

    def load_weights(at):
        slot = at % 2
        return pltpu.make_async_copy(w_ref.at[order_ref[first_pos + at]], w.at[slot], w_sem.at[slot])

    @pl.when(step == 0)
    def _():
        @pl.loop(0, srcs)
        def _(s):
            load_rows(s).start()

        load_weights(0).start()

    if steps > 1:
        @pl.when(step < steps - 1)
        def _():
            load_weights(step + 1).start()

    @pl.when(step > 0)
    def _():
        each_grad(step - 1, lambda copy: copy.wait())

    if has_prev:
        load_prev().start()
    else:
        acc[...] = jnp.zeros_like(acc)

    def pick(s):
        slot = (lax.broadcasted_iota(jnp.int32, (size, size), 0) + 1).astype(F32)
        return meta_ref[s, pl.ds(k, 1), lanes] == slot

    def gather(s, off):
        @pl.when(step == 0)
        def _():
            load_rows(s).wait()

        off = pl.multiple_of(off, ALIGN)
        offs[s] = off
        hit = pick(s)
        sel = hit.astype(F32).astype(BF16)
        gate = jnp.sum(jnp.where(hit, meta_ref[s, pl.ds(per_group + k, 1), lanes], 0.0), axis=1, keepdims=True)
        buf[pl.ds(off, size), 0:hidden] = dot(sel, xd[s, :, 0:hidden], 1, 0).astype(BF16)
        buf[pl.ds(off, size), hidden:] = (gate * dot(sel, xd[s, :, hidden:], 1, 0)).astype(BF16)
        count = jnp.max(meta_ref[s, pl.ds(k, 1), lanes]).astype(jnp.int32)
        return off + (count + ALIGN - 1) // ALIGN * ALIGN

    total = pl.multiple_of(lax.fori_loop(0, srcs, gather, jnp.int32(0)), ALIGN)
    buf[pl.ds(total, TILE), :] = jnp.zeros((TILE, width), BF16)
    if has_prev:
        load_prev().wait()
    load_weights(step).wait()
    ws = step % 2
    if sums_in:
        @pl.when(step == 0)
        def _():
            pltpu.make_async_copy(before, pq, sum_sem).start()

    @pl.loop(0, (total + TILE - 1) // TILE)
    def _(i):
        tile = pl.ds(pl.multiple_of(i * TILE, TILE), TILE)
        x = buf[tile, 0:hidden]
        d = buf[tile, hidden:]
        h = dot(x, w[ws, 0:hidden, :], 1, 0)
        da = dot(d, w[ws, hidden:, :], 1, 1)
        h1 = h[:, 0:ff]
        h3 = h[:, ff:]
        sig = jax.nn.sigmoid(h1)
        silu = h1 * sig
        a = (silu * h3).astype(BF16)
        dh1 = (da * h3 * sig * (1.0 + h1 * (1.0 - sig))).astype(BF16)
        dh3 = (da * silu).astype(BF16)
        dh = jnp.concatenate([dh1, dh3], axis=1)
        acc[0:hidden, :] += dot(x, dh, 0, 0)
        acc[hidden:, :] += dot(a, d, 0, 0)
        buf[tile, 0:hidden] = dot(a, w[ws, hidden:, :], 1, 0).astype(BF16)
        buf[tile, hidden:] = dot(dh, w[ws, 0:hidden, :], 1, 1).astype(BF16)

    each_grad(step, lambda copy: copy.start())
    if sums_in:
        @pl.when(step == 0)
        def _():
            pltpu.make_async_copy(before, pq, sum_sem).wait()

    def combine(first, last):
        @pl.loop(0, srcs)
        def _(s):
            off = pl.multiple_of(offs[s], ALIGN)
            sel = pick(s).astype(F32).astype(BF16)
            cols = jnp.transpose(meta_ref[s, :, lanes])
            lane = lax.broadcasted_iota(jnp.int32, (size, rows2), 1)
            gate = jnp.sum(jnp.where(lane == per_group + k, cols, 0.0), axis=1, keepdims=True)
            p = gate * dot(sel, buf[pl.ds(off, size), 0:hidden], 0, 0)
            q = dot(sel, buf[pl.ds(off, size), hidden:], 0, 0)
            if not first:
                p = pq[s, :, 0:hidden] + p
                q = pq[s, :, hidden:] + q
            if last and not sums_out:
                slot = s % 2

                @pl.when(s >= 2)
                def _():
                    pltpu.make_async_copy(stage.at[slot], rows_ref.at[s - 2], pq_sem.at[slot]).wait()

                stage[slot, :, 0:hidden] = p.astype(BF16)
                stage[slot, :, hidden:] = q.astype(BF16)
                pltpu.make_async_copy(stage.at[slot], rows_ref.at[s], pq_sem.at[slot]).start()
                return
            pq[s, :, 0:hidden] = p
            pq[s, :, hidden:] = q
            if last:
                pltpu.make_async_copy(pq.at[s], rows_ref.at[s], pq_out.at[s]).start()

    pq_out = xd_sem
    if steps == 1:
        combine(not sums_in, True)
    else:
        if not sums_in:
            @pl.when(step == 0)
            def _():
                combine(True, False)

        if sums_in or steps > 2:
            @pl.when((step < steps - 1) if sums_in else ((step > 0) & (step < steps - 1)))
            def _():
                combine(False, False)

        @pl.when(step == steps - 1)
        def _():
            combine(False, True)

    @pl.when(step == steps - 1)
    def _():
        if sums_out:
            for s in range(srcs):
                pltpu.make_async_copy(pq.at[s], rows_ref.at[s], pq_out.at[s]).wait()
        else:
            for s in range(max(0, srcs - 2), srcs):
                pltpu.make_async_copy(stage.at[s % 2], rows_ref.at[s], pq_sem.at[s % 2]).wait()
        each_grad(step, lambda copy: copy.wait())


def run_experts(chunk, order, positions, meta, xd, w, prev=None, sums=None, more=None):
    srcs, size, width = xd.shape
    _, rows, hidden = w.shape
    first, steps = positions[0], len(positions)
    any_spec = pl.BlockSpec(memory_space=pl.ANY)
    vmem = pl.BlockSpec(memory_space=pltpu.VMEM)
    extra = [a for a in (prev, sums) if a is not None]
    n = srcs * size // 2
    if more is None:
        grads = [jax.ShapeDtypeStruct((steps, rows, hidden), F32)]
    else:
        grads = [jax.ShapeDtypeStruct((rows, hidden // 2), F32)] * (2 * steps)
    scratch = [
        pltpu.VMEM((srcs * size + max(size, TILE), width), BF16),
        pltpu.VMEM((rows, hidden), F32),
        pltpu.VMEM((srcs, size, width), F32),
        pltpu.VMEM((srcs, size, width), BF16),
        pltpu.VMEM((2, rows, hidden), BF16),
        pltpu.SMEM((srcs,), jnp.int32),
        pltpu.SemaphoreType.DMA,
        pltpu.SemaphoreType.DMA((2,)),
        pltpu.SemaphoreType.DMA,
        pltpu.SemaphoreType.DMA((srcs,)),
        pltpu.SemaphoreType.DMA((2,)),
    ]
    if not more:
        scratch += [pltpu.VMEM((2, size, width), BF16), pltpu.SemaphoreType.DMA((2,))]
    return pl.pallas_call(
        functools.partial(expert_kernel, chunk, first, steps, prev is not None, sums is not None, bool(more)),
        grid_spec=pltpu.PrefetchScalarGridSpec(
            num_scalar_prefetch=1,
            grid=(steps,),
            in_specs=[vmem, any_spec, any_spec] + [any_spec] * len(extra),
            out_specs=[any_spec] * (1 + len(grads)),
            scratch_shapes=scratch,
        ),
        out_shape=(jax.ShapeDtypeStruct(xd.shape, F32 if more else BF16), *grads),
        compiler_params=pltpu.CompilerParams(vmem_limit_bytes=63 * 1024 * 1024, dimension_semantics=('arbitrary',)),
        cost_estimate=pl.CostEstimate(flops=steps * n * (6 * rows * hidden + 8 * size * hidden), bytes_accessed=srcs * size * width * 4, transcendentals=0),
        name='run_experts',
    )(order, meta, xd, w, *extra)


def home_kernel(first, slot_ref, ret_ref, *refs):
    refs, (ret, acc, sems) = refs[:-3], refs[-3:]
    groups, size, width = ret_ref.shape
    loads = [pltpu.make_async_copy(ret_ref.at[g], ret.at[g], sems.at[g]) for g in range(groups)]

    @pl.when(pl.program_id(0) == 0)
    def _():
        for copy in loads:
            copy.start()

    outs = refs[1:] if first else refs
    acc[...] = refs[0][...] if first else jnp.zeros_like(acc)
    slots = jnp.transpose(slot_ref[...])
    lane = lax.broadcasted_iota(jnp.int32, slots.shape, 1)
    want = (lax.broadcasted_iota(jnp.int32, (slots.shape[0], size), 1) + (first + 1)).astype(F32)

    @pl.loop(0, groups)
    def _(g):
        @pl.when(pl.program_id(0) == 0)
        def _():
            pltpu.make_async_copy(ret_ref.at[g], ret.at[g], sems.at[g]).wait()

        col = jnp.sum(jnp.where(lane == g, slots, 0.0), axis=1, keepdims=True)
        acc[...] += dot((col == want).astype(F32).astype(BF16), ret[g], 1, 0)

    if len(outs) == 1:
        outs[0][...] = acc[...]
    else:
        outs[0][...] = acc[:, :width // 2].astype(BF16)
        outs[1][...] = acc[:, width // 2:].astype(BF16)


def home_sum(slot, ret, c, before, last, block):
    groups, tokens = slot.shape
    _, size, width = ret.shape
    rows = lambda w: pl.BlockSpec((block, w), lambda i: (i, 0))
    hidden = width // 2
    outs = [(hidden, BF16)] * 2 if last else [(width, F32)]
    extra = [] if before is None else [before]
    return pl.pallas_call(
        functools.partial(home_kernel, c * size),
        grid=(tokens // block,),
        out_shape=[jax.ShapeDtypeStruct((tokens, w), t) for w, t in outs],
        in_specs=[pl.BlockSpec((groups, block), lambda i: (0, i)), pl.BlockSpec(memory_space=pl.ANY)] + [rows(width)] * len(extra),
        out_specs=[rows(w) for w, _ in outs],
        scratch_shapes=[pltpu.VMEM(ret.shape, BF16), pltpu.VMEM((block, width), F32), pltpu.SemaphoreType.DMA((groups,))],
        compiler_params=pltpu.CompilerParams(vmem_limit_bytes=58 * 1024 * 1024),
        cost_estimate=pl.CostEstimate(flops=2 * groups * size * tokens * width, bytes_accessed=groups * size * width * 2, transcendentals=0),
        name='home_sum',
    )(slot, ret, *extra)


def pair_kernel(a_ref, b_ref, c_ref, d_ref, left_ref, right_ref):
    left_ref[...] = a_ref[...] + b_ref[...]
    right_ref[...] = c_ref[...] + d_ref[...]


def pair_sums(own0, soon0, own1, soon1):
    rows, ff = own0.shape
    spec = pl.BlockSpec((ff // 2, ff), lambda i: (i, 0))
    return pl.pallas_call(
        pair_kernel,
        grid=(2 * rows // ff,),
        out_shape=[jax.ShapeDtypeStruct(own0.shape, F32)] * 2,
        in_specs=[spec] * 4,
        out_specs=[spec] * 2,
        compiler_params=pltpu.CompilerParams(vmem_limit_bytes=58 * 1024 * 1024),
        cost_estimate=pl.CostEstimate(flops=2 * rows * ff, bytes_accessed=24 * rows * ff, transcendentals=0),
        name='pair_sums',
    )(own0, soon0, own1, soon1)


def finish_kernel(a_ref, b_ref, c_ref, d_ref, g1_ref, g3_ref, g2_ref):
    tops = pl.num_programs(0) - pl.num_programs(0) // 3
    i = pl.program_id(0)
    left = a_ref[...] + b_ref[...]
    right = c_ref[...] + d_ref[...]

    @pl.when(i < tops)
    def _():
        g1_ref[0] = left
        g3_ref[0] = right

    @pl.when(i >= tops)
    def _():
        g2_ref[0] = jnp.concatenate([left, right], axis=1)


def finish(left, late0, right, late1, hidden):
    rows, ff = left.shape
    assert rows == hidden + ff and hidden == 2 * ff
    block = ff // 2
    tops = hidden // block
    top = pl.BlockSpec((1, block, ff), lambda i: (0, jnp.minimum(i, tops - 1), 0))
    return pl.pallas_call(
        finish_kernel,
        grid=(rows // block,),
        out_shape=[jax.ShapeDtypeStruct((1,) + a, F32) for a in ((hidden, ff), (hidden, ff), (ff, hidden))],
        in_specs=[pl.BlockSpec((block, ff), lambda i: (i, 0))] * 4,
        out_specs=[top, top, pl.BlockSpec((1, block, hidden), lambda i: (0, jnp.maximum(i - tops, 0), 0))],
        compiler_params=pltpu.CompilerParams(vmem_limit_bytes=16 * 1024 * 1024),
        cost_estimate=pl.CostEstimate(flops=2 * rows * ff, bytes_accessed=24 * rows * ff, transcendentals=0),
        name='finish',
    )(left, late0, right, late1)


def solution(mesh):
    groups = mesh.shape['grp']
    inner = mesh.shape['ing']
    tok_spec = P(('dp', 'grp', 'ing'), None)
    weight_spec = P(('grp', 'ing'), None, None)
    grad_spec = P(('dp', 'grp', 'ing'), None, None)
    chunks = 2

    def layer(x_loc, ids_loc, gates_loc, dy_loc, wg_loc, wu_loc, wd_loc):
        tokens, hidden = x_loc.shape
        top_k = ids_loc.shape[1]
        per_group = wg_loc.shape[0] * inner
        group_limit = min(max(1, groups // 2), top_k // 2)
        cap = tokens * group_limit // groups
        swap = lambda a: lax.all_to_all(a, 'grp', 0, 0, tiled=True)
        size = cap // chunks
        slot, meta, w_own = make_tables(ids_loc.T, gates_loc.T, (wg_loc, wu_loc, wd_loc), groups, per_group, cap, size)
        w_all = lax.all_gather(w_own, 'ing', axis=0, tiled=True)
        meta = swap(meta)
        recv = []
        for c in range(chunks):
            packed = pack_rows(slot, x_loc, dy_loc, c, size)
            if c == 0:
                packed, slot, meta = lax.optimization_barrier((packed, slot, meta))
            recv.append(swap(packed))
        me = lax.axis_index('ing')
        away = [inner // 2] + [i for i in range(1, inner) if i != inner // 2] + [0]
        order = (me + jnp.asarray(away, jnp.int32)) % inner
        everyone = list(range(per_group))
        ring = lambda a, d: lax.ppermute(a, 'ing', [(i, (i + d) % inner) for i in range(inner)])
        grads = None
        total = None
        c = chunks - 1
        rets = []
        for i in range(c):
            pq, grads = run_experts(i, order, everyone, meta, recv[i], w_all, grads)
            rets.append(swap(pq))
        sums, *far = run_experts(c, order, everyone[:1], meta, recv[c], w_all, grads, None, True)
        far0 = ring(far[0], 1)
        far1 = ring(far[1], -1)
        sums, next0, next1, last0, last1 = run_experts(c, order, everyone[1:-1], meta, recv[c], w_all, grads, sums, True)
        soon1 = ring(next1, 1)
        soon0 = ring(last0, -1)
        pq, own0, own1 = run_experts(c, order, everyone[-1:], meta, recv[c], w_all, grads, sums, False)
        rets.append(swap(pq))
        late0 = ring(next0 + far0, 1)
        late1 = ring(last1 + far1, -1)
        left, right = pair_sums(own0, soon0, own1, soon1)
        for i in range(chunks):
            total = home_sum(slot, rets[i], i, total, i == c, tokens // 2)
            total = total[0] if i < c else total
        y_out, dx_out = total
        g1, g3, g2 = finish(left, late0, right, late1, hidden)
        return y_out, dx_out, g1, g3, g2

    return jax.shard_map(layer, mesh=mesh, in_specs=(tok_spec, tok_spec, tok_spec, tok_spec, weight_spec, weight_spec, weight_spec), out_specs=(tok_spec, tok_spec, grad_spec, grad_spec, grad_spec), check_vma=False)
```

```python
import functools

import jax
import jax.numpy as jnp
from jax import lax
from jax.experimental import pallas as pl
from jax.experimental.pallas import tpu as pltpu
from jax.sharding import PartitionSpec as P


F32 = jnp.float32
BF16 = jnp.bfloat16
ALIGN = 16
TILE = 256


def dot(a, b, ca, cb):
    return lax.dot_general(a, b, (((ca,), (cb,)), ((), ())), preferred_element_type=F32)


def split3(v):
    hi = v.astype(BF16)
    rest = v - hi.astype(F32)
    mid = rest.astype(BF16)
    lo = (rest - mid.astype(F32)).astype(BF16)
    return jnp.concatenate([hi.astype(F32), mid.astype(F32), lo.astype(F32)], axis=0).astype(BF16)


def table_rows(groups, per_group, ids_ref, gates_ref, slots, vals):
    top_k, tokens = ids_ref.shape
    num_exp = groups * per_group
    exp_iota = lax.broadcasted_iota(jnp.int32, (num_exp, tokens), 0)
    grp_iota = lax.broadcasted_iota(jnp.int32, (groups, tokens), 0)
    mem = jnp.zeros((num_exp, tokens), F32)
    gate = jnp.zeros((num_exp, tokens), F32)
    gmem = jnp.zeros((groups, tokens), F32)
    for j in range(top_k):
        row = ids_ref[j:j + 1, :]
        hit = row == exp_iota
        mem = jnp.where(hit, 1.0, mem)
        gate = jnp.where(hit, gates_ref[j:j + 1, :], gate)
        gmem = jnp.where((row // per_group) == grp_iota, 1.0, gmem)
    upper = (lax.broadcasted_iota(jnp.int32, (tokens, tokens), 0) <= lax.broadcasted_iota(jnp.int32, (tokens, tokens), 1)).astype(F32).astype(BF16)
    rank = jnp.where(mem > 0, dot(mem.astype(BF16), upper, 1, 0), 0.0)
    slots[...] = jnp.where(gmem > 0, dot(gmem.astype(BF16), upper, 1, 0), 0.0)
    for g in range(groups):
        vals[g, 0:per_group, :] = rank[g * per_group:(g + 1) * per_group, :]
        vals[g, per_group:2 * per_group, :] = gate[g * per_group:(g + 1) * per_group, :]


def pick_rows(slot_row, first, count):
    want = (lax.broadcasted_iota(jnp.int32, (count, slot_row.shape[1]), 0) + (first + 1)).astype(F32)
    return (slot_row == want).astype(F32).astype(BF16)


def table_kernel(groups, per_group, size, ids_ref, gates_ref, *refs):
    weights, (slot_ref, meta_ref, joined_ref, vals, joined, sems) = refs[:3], refs[3:]
    hidden, ff = weights[0].shape[1:]
    places = ((pl.ds(0, hidden), pl.ds(0, ff)), (pl.ds(0, hidden), pl.ds(ff, ff)), (pl.ds(hidden, ff), pl.ds(0, hidden)))
    loads = [pltpu.make_async_copy(weights[i].at[0], joined.at[r, c], sems.at[i]) for i, (r, c) in enumerate(places)]
    store = pltpu.make_async_copy(joined, joined_ref.at[0], sems.at[3])
    for copy in loads:
        copy.start()
    table_rows(groups, per_group, ids_ref, gates_ref, slot_ref, vals)
    for copy in loads:
        copy.wait()
    store.start()
    n = 2 * per_group
    is_rank = lax.broadcasted_iota(jnp.int32, (n, 1), 0) < per_group

    @pl.loop(0, groups)
    def _(h):
        row = slot_ref[pl.ds(h, 1), :]
        split = split3(vals[h])
        base = jnp.zeros((n, 1), F32)
        for c in range(meta_ref.shape[2] // size):
            parts = dot(split, pick_rows(row, c * size, size), 1, 1)
            full = (parts[0:n] + parts[n:2 * n]) + parts[2 * n:3 * n]
            meta_ref[h, :, c * size:(c + 1) * size] = jnp.where(is_rank & (full > 0), full - base, full)
            base = jnp.where(is_rank, jnp.maximum(base, jnp.max(full, axis=1, keepdims=True)), 0.0)

    store.wait()


def make_tables(ids_t, gates_t, weights, groups, per_group, cap, size):
    tokens = ids_t.shape[1]
    vmem = pl.BlockSpec(memory_space=pltpu.VMEM)
    any_spec = pl.BlockSpec(memory_space=pl.ANY)
    _, hidden, ff = weights[0].shape
    assert hidden == 2 * ff and weights[2].shape == (1, ff, hidden)
    joined = (hidden + ff, hidden)
    return pl.pallas_call(
        functools.partial(table_kernel, groups, per_group, size),
        out_shape=(
            jax.ShapeDtypeStruct((groups, tokens), F32),
            jax.ShapeDtypeStruct((groups, 2 * per_group, cap), F32),
            jax.ShapeDtypeStruct((1,) + joined, BF16),
        ),
        in_specs=[vmem, vmem] + [any_spec] * 3,
        out_specs=(vmem, vmem, any_spec),
        scratch_shapes=[
            pltpu.VMEM((groups, 2 * per_group, tokens), F32),
            pltpu.VMEM(joined, BF16),
            pltpu.SemaphoreType.DMA((4,)),
        ],
        compiler_params=pltpu.CompilerParams(vmem_limit_bytes=58 * 1024 * 1024),
        cost_estimate=pl.CostEstimate(flops=2 * groups * cap * tokens * 128, bytes_accessed=groups * cap * 64, transcendentals=0),
        name='make_tables',
    )(ids_t, gates_t, *weights)


def pack_kernel(first, slot_ref, x_ref, dy_ref, packed_ref):
    size, width = packed_ref.shape[1:]
    pick = pick_rows(slot_ref[pl.ds(pl.program_id(0), 1), :], first, size)
    packed_ref[0, :, 0:width // 2] = dot(pick, x_ref[...], 1, 0).astype(BF16)
    packed_ref[0, :, width // 2:] = dot(pick, dy_ref[...], 1, 0).astype(BF16)


def pack_rows(slot, x, dy, c, size):
    groups, tokens = slot.shape
    hidden = x.shape[1]
    vmem = pl.BlockSpec(memory_space=pltpu.VMEM)
    return pl.pallas_call(
        functools.partial(pack_kernel, c * size),
        grid=(groups,),
        out_shape=jax.ShapeDtypeStruct((groups, size, 2 * hidden), BF16),
        in_specs=[vmem, vmem, vmem],
        out_specs=pl.BlockSpec((1, size, 2 * hidden), lambda h: (h, 0, 0)),
        compiler_params=pltpu.CompilerParams(vmem_limit_bytes=58 * 1024 * 1024),
        cost_estimate=pl.CostEstimate(flops=4 * groups * size * tokens * hidden, bytes_accessed=groups * size * hidden * 4, transcendentals=0),
        name='pack_rows',
    )(slot, x, dy)


def expert_kernel(chunk, first_pos, steps, has_prev, sums_in, sums_out, order_ref, meta_ref, xd_ref, w_ref, *refs):
    refs = list(refs)
    prev = refs.pop(0) if has_prev else None
    before = refs.pop(0) if sums_in else None
    rows_ref = refs.pop(0)
    split = sums_in or sums_out
    grad_refs = [refs.pop(0) for _ in range(2 * steps if split else 1)]
    buf, acc, pq, xd, w, offs, in_sem, out_sem, sum_sem, xd_sem, w_sem = refs[:11]
    stage, pq_sem = (None, None) if sums_out else refs[11:]
    step = pl.program_id(0)
    k = order_ref[first_pos + step]
    srcs, size, width = xd_ref.shape
    hidden = width // 2
    rows2 = meta_ref.shape[1]
    per_group = rows2 // 2
    ff = acc.shape[0] - hidden
    lanes = pl.ds(chunk * size, size)

    def each_grad(at, act):
        if not split:
            act(pltpu.make_async_copy(acc, grad_refs[0].at[at], out_sem.at[0]))
            return
        for i in range(steps):
            @pl.when(at == i)
            def _(i=i):
                for j in range(2):
                    act(pltpu.make_async_copy(acc.at[:, pl.ds(j * ff, ff)], grad_refs[2 * i + j], out_sem.at[j]))

    def load_prev():
        return pltpu.make_async_copy(prev.at[first_pos + step], acc, in_sem)

    def load_rows(s):
        return pltpu.make_async_copy(xd_ref.at[s], xd.at[s], xd_sem.at[s])

    def load_weights(at):
        slot = at % 2
        return pltpu.make_async_copy(w_ref.at[order_ref[first_pos + at]], w.at[slot], w_sem.at[slot])

    @pl.when(step == 0)
    def _():
        @pl.loop(0, srcs)
        def _(s):
            load_rows(s).start()

        load_weights(0).start()

    if steps > 1:
        @pl.when(step < steps - 1)
        def _():
            load_weights(step + 1).start()

    @pl.when(step > 0)
    def _():
        each_grad(step - 1, lambda copy: copy.wait())

    if has_prev:
        load_prev().start()
    else:
        acc[...] = jnp.zeros_like(acc)

    def pick(s):
        slot = (lax.broadcasted_iota(jnp.int32, (size, size), 0) + 1).astype(F32)
        return meta_ref[s, pl.ds(k, 1), lanes] == slot

    def gather(s, off):
        @pl.when(step == 0)
        def _():
            load_rows(s).wait()

        off = pl.multiple_of(off, ALIGN)
        offs[s] = off
        hit = pick(s)
        sel = hit.astype(F32).astype(BF16)
        gate = jnp.sum(jnp.where(hit, meta_ref[s, pl.ds(per_group + k, 1), lanes], 0.0), axis=1, keepdims=True)
        buf[pl.ds(off, size), 0:hidden] = dot(sel, xd[s, :, 0:hidden], 1, 0).astype(BF16)
        buf[pl.ds(off, size), hidden:] = (gate * dot(sel, xd[s, :, hidden:], 1, 0)).astype(BF16)
        count = jnp.max(meta_ref[s, pl.ds(k, 1), lanes]).astype(jnp.int32)
        return off + (count + ALIGN - 1) // ALIGN * ALIGN

    total = pl.multiple_of(lax.fori_loop(0, srcs, gather, jnp.int32(0)), ALIGN)
    buf[pl.ds(total, TILE), :] = jnp.zeros((TILE, width), BF16)
    if has_prev:
        load_prev().wait()
    load_weights(step).wait()
    ws = step % 2
    if sums_in:
        @pl.when(step == 0)
        def _():
            pltpu.make_async_copy(before, pq, sum_sem).start()

    @pl.loop(0, (total + TILE - 1) // TILE)
    def _(i):
        tile = pl.ds(pl.multiple_of(i * TILE, TILE), TILE)
        x = buf[tile, 0:hidden]
        d = buf[tile, hidden:]
        h = dot(x, w[ws, 0:hidden, :], 1, 0)
        da = dot(d, w[ws, hidden:, :], 1, 1)
        h1 = h[:, 0:ff]
        h3 = h[:, ff:]
        sig = jax.nn.sigmoid(h1)
        silu = h1 * sig
        a = (silu * h3).astype(BF16)
        dh1 = (da * h3 * sig * (1.0 + h1 * (1.0 - sig))).astype(BF16)
        dh3 = (da * silu).astype(BF16)
        dh = jnp.concatenate([dh1, dh3], axis=1)
        acc[0:hidden, :] += dot(x, dh, 0, 0)
        acc[hidden:, :] += dot(a, d, 0, 0)
        buf[tile, 0:hidden] = dot(a, w[ws, hidden:, :], 1, 0).astype(BF16)
        buf[tile, hidden:] = dot(dh, w[ws, 0:hidden, :], 1, 1).astype(BF16)

    each_grad(step, lambda copy: copy.start())
    if sums_in:
        @pl.when(step == 0)
        def _():
            pltpu.make_async_copy(before, pq, sum_sem).wait()

    def combine(first, last):
        @pl.loop(0, srcs)
        def _(s):
            off = pl.multiple_of(offs[s], ALIGN)
            sel = pick(s).astype(F32).astype(BF16)
            cols = jnp.transpose(meta_ref[s, :, lanes])
            lane = lax.broadcasted_iota(jnp.int32, (size, rows2), 1)
            gate = jnp.sum(jnp.where(lane == per_group + k, cols, 0.0), axis=1, keepdims=True)
            p = gate * dot(sel, buf[pl.ds(off, size), 0:hidden], 0, 0)
            q = dot(sel, buf[pl.ds(off, size), hidden:], 0, 0)
            if not first:
                p = pq[s, :, 0:hidden] + p
                q = pq[s, :, hidden:] + q
            if last and not sums_out:
                slot = s % 2

                @pl.when(s >= 2)
                def _():
                    pltpu.make_async_copy(stage.at[slot], rows_ref.at[s - 2], pq_sem.at[slot]).wait()

                stage[slot, :, 0:hidden] = p.astype(BF16)
                stage[slot, :, hidden:] = q.astype(BF16)
                pltpu.make_async_copy(stage.at[slot], rows_ref.at[s], pq_sem.at[slot]).start()
                return
            pq[s, :, 0:hidden] = p
            pq[s, :, hidden:] = q
            if last:
                pltpu.make_async_copy(pq.at[s], rows_ref.at[s], pq_out.at[s]).start()

    pq_out = xd_sem
    if steps == 1:
        combine(not sums_in, True)
    else:
        if not sums_in:
            @pl.when(step == 0)
            def _():
                combine(True, False)

        if sums_in or steps > 2:
            @pl.when((step < steps - 1) if sums_in else ((step > 0) & (step < steps - 1)))
            def _():
                combine(False, False)

        @pl.when(step == steps - 1)
        def _():
            combine(False, True)

    @pl.when(step == steps - 1)
    def _():
        if sums_out:
            for s in range(srcs):
                pltpu.make_async_copy(pq.at[s], rows_ref.at[s], pq_out.at[s]).wait()
        else:
            for s in range(max(0, srcs - 2), srcs):
                pltpu.make_async_copy(stage.at[s % 2], rows_ref.at[s], pq_sem.at[s % 2]).wait()
        each_grad(step, lambda copy: copy.wait())


def run_experts(chunk, order, positions, meta, xd, w, prev=None, sums=None, more=None):
    srcs, size, width = xd.shape
    _, rows, hidden = w.shape
    first, steps = positions[0], len(positions)
    any_spec = pl.BlockSpec(memory_space=pl.ANY)
    vmem = pl.BlockSpec(memory_space=pltpu.VMEM)
    extra = [a for a in (prev, sums) if a is not None]
    n = srcs * size // 2
    if more is None:
        grads = [jax.ShapeDtypeStruct((steps, rows, hidden), F32)]
    else:
        grads = [jax.ShapeDtypeStruct((rows, hidden // 2), F32)] * (2 * steps)
    scratch = [
        pltpu.VMEM((srcs * size + max(size, TILE), width), BF16),
        pltpu.VMEM((rows, hidden), F32),
        pltpu.VMEM((srcs, size, width), F32),
        pltpu.VMEM((srcs, size, width), BF16),
        pltpu.VMEM((2, rows, hidden), BF16),
        pltpu.SMEM((srcs,), jnp.int32),
        pltpu.SemaphoreType.DMA,
        pltpu.SemaphoreType.DMA((2,)),
        pltpu.SemaphoreType.DMA,
        pltpu.SemaphoreType.DMA((srcs,)),
        pltpu.SemaphoreType.DMA((2,)),
    ]
    if not more:
        scratch += [pltpu.VMEM((2, size, width), BF16), pltpu.SemaphoreType.DMA((2,))]
    return pl.pallas_call(
        functools.partial(expert_kernel, chunk, first, steps, prev is not None, sums is not None, bool(more)),
        grid_spec=pltpu.PrefetchScalarGridSpec(
            num_scalar_prefetch=1,
            grid=(steps,),
            in_specs=[vmem, any_spec, any_spec] + [any_spec] * len(extra),
            out_specs=[any_spec] * (1 + len(grads)),
            scratch_shapes=scratch,
        ),
        out_shape=(jax.ShapeDtypeStruct(xd.shape, F32 if more else BF16), *grads),
        compiler_params=pltpu.CompilerParams(vmem_limit_bytes=63 * 1024 * 1024, dimension_semantics=('arbitrary',)),
        cost_estimate=pl.CostEstimate(flops=steps * n * (6 * rows * hidden + 8 * size * hidden), bytes_accessed=srcs * size * width * 4, transcendentals=0),
        name='run_experts',
    )(order, meta, xd, w, *extra)


def home_kernel(first, slot_ref, ret_ref, *refs):
    refs, (ret, sems) = refs[:-2], refs[-2:]
    groups, size, width = ret_ref.shape
    loads = [pltpu.make_async_copy(ret_ref.at[g], ret.at[g], sems.at[g]) for g in range(groups)]

    @pl.when(pl.program_id(0) == 0)
    def _():
        for copy in loads:
            copy.start()

    outs = refs[1:] if first else refs
    acc = refs[0][...] if first else None
    for g in range(groups):
        @pl.when(pl.program_id(0) == 0)
        def _(g=g):
            loads[g].wait()

        part = dot(pick_rows(slot_ref[g:g + 1, :], first, size), ret[g], 0, 0)
        acc = part if acc is None else acc + part
    if len(outs) == 1:
        outs[0][...] = acc
    else:
        outs[0][...] = acc[:, :width // 2].astype(BF16)
        outs[1][...] = acc[:, width // 2:].astype(BF16)


def home_sum(slot, ret, c, before, last, block):
    groups, tokens = slot.shape
    _, size, width = ret.shape
    rows = lambda w: pl.BlockSpec((block, w), lambda i: (i, 0))
    hidden = width // 2
    outs = [(hidden, BF16)] * 2 if last else [(width, F32)]
    extra = [] if before is None else [before]
    return pl.pallas_call(
        functools.partial(home_kernel, c * size),
        grid=(tokens // block,),
        out_shape=[jax.ShapeDtypeStruct((tokens, w), t) for w, t in outs],
        in_specs=[pl.BlockSpec((groups, block), lambda i: (0, i)), pl.BlockSpec(memory_space=pl.ANY)] + [rows(width)] * len(extra),
        out_specs=[rows(w) for w, _ in outs],
        scratch_shapes=[pltpu.VMEM(ret.shape, BF16), pltpu.SemaphoreType.DMA((groups,))],
        compiler_params=pltpu.CompilerParams(vmem_limit_bytes=58 * 1024 * 1024),
        cost_estimate=pl.CostEstimate(flops=2 * groups * size * tokens * width, bytes_accessed=groups * size * width * 2, transcendentals=0),
        name='home_sum',
    )(slot, ret, *extra)


def pair_kernel(a_ref, b_ref, c_ref, d_ref, left_ref, right_ref):
    left_ref[...] = a_ref[...] + b_ref[...]
    right_ref[...] = c_ref[...] + d_ref[...]


def pair_sums(own0, soon0, own1, soon1):
    rows, ff = own0.shape
    spec = pl.BlockSpec((ff // 2, ff), lambda i: (i, 0))
    return pl.pallas_call(
        pair_kernel,
        grid=(2 * rows // ff,),
        out_shape=[jax.ShapeDtypeStruct(own0.shape, F32)] * 2,
        in_specs=[spec] * 4,
        out_specs=[spec] * 2,
        compiler_params=pltpu.CompilerParams(vmem_limit_bytes=58 * 1024 * 1024),
        cost_estimate=pl.CostEstimate(flops=2 * rows * ff, bytes_accessed=24 * rows * ff, transcendentals=0),
        name='pair_sums',
    )(own0, soon0, own1, soon1)


def finish_kernel(a_ref, b_ref, c_ref, d_ref, g1_ref, g3_ref, g2_ref):
    tops = pl.num_programs(0) - pl.num_programs(0) // 3
    i = pl.program_id(0)
    left = a_ref[...] + b_ref[...]
    right = c_ref[...] + d_ref[...]

    @pl.when(i < tops)
    def _():
        g1_ref[0] = left
        g3_ref[0] = right

    @pl.when(i >= tops)
    def _():
        g2_ref[0] = jnp.concatenate([left, right], axis=1)


def finish(left, late0, right, late1, hidden):
    rows, ff = left.shape
    assert rows == hidden + ff and hidden == 2 * ff
    block = ff // 2
    tops = hidden // block
    top = pl.BlockSpec((1, block, ff), lambda i: (0, jnp.minimum(i, tops - 1), 0))
    return pl.pallas_call(
        finish_kernel,
        grid=(rows // block,),
        out_shape=[jax.ShapeDtypeStruct((1,) + a, F32) for a in ((hidden, ff), (hidden, ff), (ff, hidden))],
        in_specs=[pl.BlockSpec((block, ff), lambda i: (i, 0))] * 4,
        out_specs=[top, top, pl.BlockSpec((1, block, hidden), lambda i: (0, jnp.maximum(i - tops, 0), 0))],
        compiler_params=pltpu.CompilerParams(vmem_limit_bytes=58 * 1024 * 1024),
        cost_estimate=pl.CostEstimate(flops=2 * rows * ff, bytes_accessed=24 * rows * ff, transcendentals=0),
        name='finish',
    )(left, late0, right, late1)


def solution(mesh):
    groups = mesh.shape['grp']
    inner = mesh.shape['ing']
    tok_spec = P(('dp', 'grp', 'ing'), None)
    weight_spec = P(('grp', 'ing'), None, None)
    grad_spec = P(('dp', 'grp', 'ing'), None, None)
    chunks = 2

    def layer(x_loc, ids_loc, gates_loc, dy_loc, wg_loc, wu_loc, wd_loc):
        tokens, hidden = x_loc.shape
        top_k = ids_loc.shape[1]
        per_group = wg_loc.shape[0] * inner
        group_limit = min(max(1, groups // 2), top_k // 2)
        cap = tokens * group_limit // groups
        swap = lambda a: lax.all_to_all(a, 'grp', 0, 0, tiled=True)
        size = cap // chunks
        slot, meta, w_own = make_tables(ids_loc.T, gates_loc.T, (wg_loc, wu_loc, wd_loc), groups, per_group, cap, size)
        w_all = lax.all_gather(w_own, 'ing', axis=0, tiled=True)
        meta = swap(meta)
        recv = []
        for c in range(chunks):
            packed = pack_rows(slot, x_loc, dy_loc, c, size)
            if c == 0:
                packed, slot, meta = lax.optimization_barrier((packed, slot, meta))
            recv.append(swap(packed))
        me = lax.axis_index('ing')
        away = [inner // 2] + [i for i in range(1, inner) if i != inner // 2] + [0]
        order = (me + jnp.asarray(away, jnp.int32)) % inner
        everyone = list(range(per_group))
        ring = lambda a, d: lax.ppermute(a, 'ing', [(i, (i + d) % inner) for i in range(inner)])
        grads = None
        total = None
        c = chunks - 1
        rets = []
        for i in range(c):
            pq, grads = run_experts(i, order, everyone, meta, recv[i], w_all, grads)
            rets.append(swap(pq))
        sums, *far = run_experts(c, order, everyone[:1], meta, recv[c], w_all, grads, None, True)
        far0 = ring(far[0], 1)
        far1 = ring(far[1], -1)
        sums, next0, next1, last0, last1 = run_experts(c, order, everyone[1:-1], meta, recv[c], w_all, grads, sums, True)
        soon1 = ring(next1, 1)
        soon0 = ring(last0, -1)
        pq, own0, own1 = run_experts(c, order, everyone[-1:], meta, recv[c], w_all, grads, sums, False)
        rets.append(swap(pq))
        late0 = ring(next0 + far0, 1)
        late1 = ring(last1 + far1, -1)
        left, right = pair_sums(own0, soon0, own1, soon1)
        for i in range(chunks):
            total = home_sum(slot, rets[i], i, total, i == c, tokens // 4)
            total = total[0] if i < c else total
        y_out, dx_out = total
        g1, g3, g2 = finish(left, late0, right, late1, hidden)
        return y_out, dx_out, g1, g3, g2

    return jax.shard_map(layer, mesh=mesh, in_specs=(tok_spec, tok_spec, tok_spec, tok_spec, weight_spec, weight_spec, weight_spec), out_specs=(tok_spec, tok_spec, grad_spec, grad_spec, grad_spec), check_vma=False)
```

```python
import functools

import jax
import jax.numpy as jnp
from jax import lax
from jax.experimental import pallas as pl
from jax.experimental.pallas import tpu as pltpu
from jax.sharding import PartitionSpec as P


F32 = jnp.float32
BF16 = jnp.bfloat16
ALIGN = 16
TILE = 256


def dot(a, b, ca, cb):
    return lax.dot_general(a, b, (((ca,), (cb,)), ((), ())), preferred_element_type=F32)


def split3(v):
    hi = v.astype(BF16)
    rest = v - hi.astype(F32)
    mid = rest.astype(BF16)
    lo = (rest - mid.astype(F32)).astype(BF16)
    return jnp.concatenate([hi.astype(F32), mid.astype(F32), lo.astype(F32)], axis=0).astype(BF16)


def table_rows(groups, per_group, ids_ref, gates_ref, slots, vals):
    top_k, tokens = ids_ref.shape
    num_exp = groups * per_group
    exp_iota = lax.broadcasted_iota(jnp.int32, (num_exp, tokens), 0)
    grp_iota = lax.broadcasted_iota(jnp.int32, (groups, tokens), 0)
    mem = jnp.zeros((num_exp, tokens), F32)
    gate = jnp.zeros((num_exp, tokens), F32)
    gmem = jnp.zeros((groups, tokens), F32)
    for j in range(top_k):
        row = ids_ref[j:j + 1, :]
        hit = row == exp_iota
        mem = jnp.where(hit, 1.0, mem)
        gate = jnp.where(hit, gates_ref[j:j + 1, :], gate)
        gmem = jnp.where((row // per_group) == grp_iota, 1.0, gmem)
    upper = (lax.broadcasted_iota(jnp.int32, (tokens, tokens), 0) <= lax.broadcasted_iota(jnp.int32, (tokens, tokens), 1)).astype(F32).astype(BF16)
    rank = jnp.where(mem > 0, dot(mem.astype(BF16), upper, 1, 0), 0.0)
    slots[...] = jnp.where(gmem > 0, dot(gmem.astype(BF16), upper, 1, 0), 0.0)
    for g in range(groups):
        vals[g, 0:per_group, :] = rank[g * per_group:(g + 1) * per_group, :]
        vals[g, per_group:2 * per_group, :] = gate[g * per_group:(g + 1) * per_group, :]


def pick_rows(slot_row, first, count):
    want = (lax.broadcasted_iota(jnp.int32, (count, slot_row.shape[1]), 0) + (first + 1)).astype(F32)
    return (slot_row == want).astype(F32).astype(BF16)


def table_kernel(groups, per_group, size, ids_ref, gates_ref, *refs):
    weights, (slot_ref, meta_ref, joined_ref, vals, joined, sems) = refs[:3], refs[3:]
    hidden, ff = weights[0].shape[1:]
    places = ((pl.ds(0, hidden), pl.ds(0, ff)), (pl.ds(0, hidden), pl.ds(ff, ff)), (pl.ds(hidden, ff), pl.ds(0, hidden)))
    loads = [pltpu.make_async_copy(weights[i].at[0], joined.at[r, c], sems.at[i]) for i, (r, c) in enumerate(places)]
    store = pltpu.make_async_copy(joined, joined_ref.at[0], sems.at[3])
    for copy in loads:
        copy.start()
    table_rows(groups, per_group, ids_ref, gates_ref, slot_ref, vals)
    for copy in loads:
        copy.wait()
    store.start()
    n = 2 * per_group
    is_rank = lax.broadcasted_iota(jnp.int32, (n, 1), 0) < per_group

    @pl.loop(0, groups)
    def _(h):
        row = slot_ref[pl.ds(h, 1), :]
        split = split3(vals[h])
        base = jnp.zeros((n, 1), F32)
        for c in range(meta_ref.shape[2] // size):
            parts = dot(split, pick_rows(row, c * size, size), 1, 1)
            full = (parts[0:n] + parts[n:2 * n]) + parts[2 * n:3 * n]
            meta_ref[h, :, c * size:(c + 1) * size] = jnp.where(is_rank & (full > 0), full - base, full)
            base = jnp.where(is_rank, jnp.maximum(base, jnp.max(full, axis=1, keepdims=True)), 0.0)

    store.wait()


def make_tables(ids_t, gates_t, weights, groups, per_group, cap, size):
    tokens = ids_t.shape[1]
    vmem = pl.BlockSpec(memory_space=pltpu.VMEM)
    any_spec = pl.BlockSpec(memory_space=pl.ANY)
    _, hidden, ff = weights[0].shape
    assert hidden == 2 * ff and weights[2].shape == (1, ff, hidden)
    joined = (hidden + ff, hidden)
    return pl.pallas_call(
        functools.partial(table_kernel, groups, per_group, size),
        out_shape=(
            jax.ShapeDtypeStruct((groups, tokens), F32),
            jax.ShapeDtypeStruct((groups, 2 * per_group, cap), F32),
            jax.ShapeDtypeStruct((1,) + joined, BF16),
        ),
        in_specs=[vmem, vmem] + [any_spec] * 3,
        out_specs=(vmem, vmem, any_spec),
        scratch_shapes=[
            pltpu.VMEM((groups, 2 * per_group, tokens), F32),
            pltpu.VMEM(joined, BF16),
            pltpu.SemaphoreType.DMA((4,)),
        ],
        compiler_params=pltpu.CompilerParams(vmem_limit_bytes=58 * 1024 * 1024),
        cost_estimate=pl.CostEstimate(flops=2 * groups * cap * tokens * 128, bytes_accessed=groups * cap * 64, transcendentals=0),
        name='make_tables',
    )(ids_t, gates_t, *weights)


def pack_kernel(first, slot_ref, x_ref, dy_ref, packed_ref):
    size, width = packed_ref.shape[1:]
    pick = pick_rows(slot_ref[pl.ds(pl.program_id(0), 1), :], first, size)
    packed_ref[0, :, 0:width // 2] = dot(pick, x_ref[...], 1, 0).astype(BF16)
    packed_ref[0, :, width // 2:] = dot(pick, dy_ref[...], 1, 0).astype(BF16)


def pack_rows(slot, x, dy, c, size):
    groups, tokens = slot.shape
    hidden = x.shape[1]
    vmem = pl.BlockSpec(memory_space=pltpu.VMEM)
    return pl.pallas_call(
        functools.partial(pack_kernel, c * size),
        grid=(groups,),
        out_shape=jax.ShapeDtypeStruct((groups, size, 2 * hidden), BF16),
        in_specs=[vmem, vmem, vmem],
        out_specs=pl.BlockSpec((1, size, 2 * hidden), lambda h: (h, 0, 0)),
        compiler_params=pltpu.CompilerParams(vmem_limit_bytes=58 * 1024 * 1024),
        cost_estimate=pl.CostEstimate(flops=4 * groups * size * tokens * hidden, bytes_accessed=groups * size * hidden * 4, transcendentals=0),
        name='pack_rows',
    )(slot, x, dy)


def expert_kernel(chunk, first_pos, steps, has_prev, sums_in, sums_out, order_ref, meta_ref, xd_ref, w_ref, *refs):
    refs = list(refs)
    prev = refs.pop(0) if has_prev else None
    before = refs.pop(0) if sums_in else None
    rows_ref = refs.pop(0)
    split = sums_in or sums_out
    grad_refs = [refs.pop(0) for _ in range(2 * steps if split else 1)]
    buf, acc, pq, xd, w, offs, in_sem, out_sem, sum_sem, xd_sem, w_sem = refs[:11]
    stage, pq_sem = (None, None) if sums_out else refs[11:]
    step = pl.program_id(0)
    k = order_ref[first_pos + step]
    srcs, size, width = xd_ref.shape
    hidden = width // 2
    rows2 = meta_ref.shape[1]
    per_group = rows2 // 2
    ff = acc.shape[0] - hidden
    lanes = pl.ds(chunk * size, size)

    def each_grad(at, act):
        if not split:
            act(pltpu.make_async_copy(acc, grad_refs[0].at[at], out_sem.at[0]))
            return
        for i in range(steps):
            @pl.when(at == i)
            def _(i=i):
                for j in range(2):
                    act(pltpu.make_async_copy(acc.at[:, pl.ds(j * ff, ff)], grad_refs[2 * i + j], out_sem.at[j]))

    def load_prev():
        return pltpu.make_async_copy(prev.at[first_pos + step], acc, in_sem)

    def load_rows(s):
        return pltpu.make_async_copy(xd_ref.at[s], xd.at[s], xd_sem.at[s])

    def load_weights(at):
        slot = at % 2
        return pltpu.make_async_copy(w_ref.at[order_ref[first_pos + at]], w.at[slot], w_sem.at[slot])

    @pl.when(step == 0)
    def _():
        @pl.loop(0, srcs)
        def _(s):
            load_rows(s).start()

        load_weights(0).start()

    if steps > 1:
        @pl.when(step < steps - 1)
        def _():
            load_weights(step + 1).start()

    @pl.when(step > 0)
    def _():
        each_grad(step - 1, lambda copy: copy.wait())

    if has_prev:
        load_prev().start()
    else:
        acc[...] = jnp.zeros_like(acc)

    def pick(s):
        slot = (lax.broadcasted_iota(jnp.int32, (size, size), 0) + 1).astype(F32)
        return meta_ref[s, pl.ds(k, 1), lanes] == slot

    def gather(s, off):
        @pl.when(step == 0)
        def _():
            load_rows(s).wait()

        off = pl.multiple_of(off, ALIGN)
        offs[s] = off
        hit = pick(s)
        sel = hit.astype(F32).astype(BF16)
        gate = jnp.sum(jnp.where(hit, meta_ref[s, pl.ds(per_group + k, 1), lanes], 0.0), axis=1, keepdims=True)
        buf[pl.ds(off, size), 0:hidden] = dot(sel, xd[s, :, 0:hidden], 1, 0).astype(BF16)
        buf[pl.ds(off, size), hidden:] = (gate * dot(sel, xd[s, :, hidden:], 1, 0)).astype(BF16)
        count = jnp.max(meta_ref[s, pl.ds(k, 1), lanes]).astype(jnp.int32)
        return off + (count + ALIGN - 1) // ALIGN * ALIGN

    total = pl.multiple_of(lax.fori_loop(0, srcs, gather, jnp.int32(0)), ALIGN)
    buf[pl.ds(total, TILE), :] = jnp.zeros((TILE, width), BF16)
    if has_prev:
        load_prev().wait()
    load_weights(step).wait()
    ws = step % 2
    if sums_in:
        @pl.when(step == 0)
        def _():
            pltpu.make_async_copy(before, pq, sum_sem).start()

    @pl.loop(0, (total + TILE - 1) // TILE)
    def _(i):
        tile = pl.ds(pl.multiple_of(i * TILE, TILE), TILE)
        x = buf[tile, 0:hidden]
        d = buf[tile, hidden:]
        h = dot(x, w[ws, 0:hidden, :], 1, 0)
        da = dot(d, w[ws, hidden:, :], 1, 1)
        h1 = h[:, 0:ff]
        h3 = h[:, ff:]
        sig = jax.nn.sigmoid(h1)
        silu = h1 * sig
        a = (silu * h3).astype(BF16)
        dh1 = (da * h3 * sig * (1.0 + h1 * (1.0 - sig))).astype(BF16)
        dh3 = (da * silu).astype(BF16)
        dh = jnp.concatenate([dh1, dh3], axis=1)
        acc[0:hidden, :] += dot(x, dh, 0, 0)
        acc[hidden:, :] += dot(a, d, 0, 0)
        buf[tile, 0:hidden] = dot(a, w[ws, hidden:, :], 1, 0).astype(BF16)
        buf[tile, hidden:] = dot(dh, w[ws, 0:hidden, :], 1, 1).astype(BF16)

    each_grad(step, lambda copy: copy.start())
    if sums_in:
        @pl.when(step == 0)
        def _():
            pltpu.make_async_copy(before, pq, sum_sem).wait()

    def combine(first, last):
        @pl.loop(0, srcs)
        def _(s):
            off = pl.multiple_of(offs[s], ALIGN)
            sel = pick(s).astype(F32).astype(BF16)
            cols = jnp.transpose(meta_ref[s, :, lanes])
            lane = lax.broadcasted_iota(jnp.int32, (size, rows2), 1)
            gate = jnp.sum(jnp.where(lane == per_group + k, cols, 0.0), axis=1, keepdims=True)
            p = gate * dot(sel, buf[pl.ds(off, size), 0:hidden], 0, 0)
            q = dot(sel, buf[pl.ds(off, size), hidden:], 0, 0)
            if not first:
                p = pq[s, :, 0:hidden] + p
                q = pq[s, :, hidden:] + q
            if last and not sums_out:
                slot = s % 2

                @pl.when(s >= 2)
                def _():
                    pltpu.make_async_copy(stage.at[slot], rows_ref.at[s - 2], pq_sem.at[slot]).wait()

                stage[slot, :, 0:hidden] = p.astype(BF16)
                stage[slot, :, hidden:] = q.astype(BF16)
                pltpu.make_async_copy(stage.at[slot], rows_ref.at[s], pq_sem.at[slot]).start()
                return
            pq[s, :, 0:hidden] = p
            pq[s, :, hidden:] = q
            if last:
                pltpu.make_async_copy(pq.at[s], rows_ref.at[s], pq_out.at[s]).start()

    pq_out = xd_sem
    if steps == 1:
        combine(not sums_in, True)
    else:
        if not sums_in:
            @pl.when(step == 0)
            def _():
                combine(True, False)

        if sums_in or steps > 2:
            @pl.when((step < steps - 1) if sums_in else ((step > 0) & (step < steps - 1)))
            def _():
                combine(False, False)

        @pl.when(step == steps - 1)
        def _():
            combine(False, True)

    @pl.when(step == steps - 1)
    def _():
        if sums_out:
            for s in range(srcs):
                pltpu.make_async_copy(pq.at[s], rows_ref.at[s], pq_out.at[s]).wait()
        else:
            for s in range(max(0, srcs - 2), srcs):
                pltpu.make_async_copy(stage.at[s % 2], rows_ref.at[s], pq_sem.at[s % 2]).wait()
        each_grad(step, lambda copy: copy.wait())


def run_experts(chunk, order, positions, meta, xd, w, prev=None, sums=None, more=None):
    srcs, size, width = xd.shape
    _, rows, hidden = w.shape
    first, steps = positions[0], len(positions)
    any_spec = pl.BlockSpec(memory_space=pl.ANY)
    vmem = pl.BlockSpec(memory_space=pltpu.VMEM)
    extra = [a for a in (prev, sums) if a is not None]
    n = srcs * size // 2
    if more is None:
        grads = [jax.ShapeDtypeStruct((steps, rows, hidden), F32)]
    else:
        grads = [jax.ShapeDtypeStruct((rows, hidden // 2), F32)] * (2 * steps)
    scratch = [
        pltpu.VMEM((srcs * size + max(size, TILE), width), BF16),
        pltpu.VMEM((rows, hidden), F32),
        pltpu.VMEM((srcs, size, width), F32),
        pltpu.VMEM((srcs, size, width), BF16),
        pltpu.VMEM((2, rows, hidden), BF16),
        pltpu.SMEM((srcs,), jnp.int32),
        pltpu.SemaphoreType.DMA,
        pltpu.SemaphoreType.DMA((2,)),
        pltpu.SemaphoreType.DMA,
        pltpu.SemaphoreType.DMA((srcs,)),
        pltpu.SemaphoreType.DMA((2,)),
    ]
    if not more:
        scratch += [pltpu.VMEM((2, size, width), BF16), pltpu.SemaphoreType.DMA((2,))]
    return pl.pallas_call(
        functools.partial(expert_kernel, chunk, first, steps, prev is not None, sums is not None, bool(more)),
        grid_spec=pltpu.PrefetchScalarGridSpec(
            num_scalar_prefetch=1,
            grid=(steps,),
            in_specs=[vmem, any_spec, any_spec] + [any_spec] * len(extra),
            out_specs=[any_spec] * (1 + len(grads)),
            scratch_shapes=scratch,
        ),
        out_shape=(jax.ShapeDtypeStruct(xd.shape, F32 if more else BF16), *grads),
        compiler_params=pltpu.CompilerParams(vmem_limit_bytes=63 * 1024 * 1024, dimension_semantics=('arbitrary',)),
        cost_estimate=pl.CostEstimate(flops=steps * n * (6 * rows * hidden + 8 * size * hidden), bytes_accessed=srcs * size * width * 4, transcendentals=0),
        name='run_experts',
    )(order, meta, xd, w, *extra)


def home_kernel(first, slot_ref, ret_ref, *refs):
    groups, size, width = ret_ref.shape
    acc = refs[0][...] if first else None
    outs = refs[1:] if first else refs
    for g in range(groups):
        part = dot(pick_rows(slot_ref[g:g + 1, :], first, size), ret_ref[g], 0, 0)
        acc = part if acc is None else acc + part
    if len(outs) == 1:
        outs[0][...] = acc
    else:
        outs[0][...] = acc[:, :width // 2].astype(BF16)
        outs[1][...] = acc[:, width // 2:].astype(BF16)


def home_sum(slot, ret, c, before, last, block):
    groups, tokens = slot.shape
    _, size, width = ret.shape
    rows = lambda w: pl.BlockSpec((block, w), lambda i: (i, 0))
    hidden = width // 2
    outs = [(hidden, BF16)] * 2 if last else [(width, F32)]
    extra = [] if before is None else [before]
    return pl.pallas_call(
        functools.partial(home_kernel, c * size),
        grid=(tokens // block,),
        out_shape=[jax.ShapeDtypeStruct((tokens, w), t) for w, t in outs],
        in_specs=[pl.BlockSpec((groups, block), lambda i: (0, i)), pl.BlockSpec(memory_space=pltpu.VMEM)] + [rows(width)] * len(extra),
        out_specs=[rows(w) for w, _ in outs],
        compiler_params=pltpu.CompilerParams(vmem_limit_bytes=48 * 1024 * 1024),
        cost_estimate=pl.CostEstimate(flops=2 * groups * size * tokens * width, bytes_accessed=groups * size * width * 2, transcendentals=0),
        name='home_sum',
    )(slot, ret, *extra)


def pair_kernel(a_ref, b_ref, c_ref, d_ref, left_ref, right_ref):
    left_ref[...] = a_ref[...] + b_ref[...]
    right_ref[...] = c_ref[...] + d_ref[...]


def pair_sums(own0, soon0, own1, soon1):
    rows, ff = own0.shape
    spec = pl.BlockSpec((ff // 2, ff), lambda i: (i, 0))
    return pl.pallas_call(
        pair_kernel,
        grid=(2 * rows // ff,),
        out_shape=[jax.ShapeDtypeStruct(own0.shape, F32)] * 2,
        in_specs=[spec] * 4,
        out_specs=[spec] * 2,
        compiler_params=pltpu.CompilerParams(vmem_limit_bytes=58 * 1024 * 1024),
        cost_estimate=pl.CostEstimate(flops=2 * rows * ff, bytes_accessed=24 * rows * ff, transcendentals=0),
        name='pair_sums',
    )(own0, soon0, own1, soon1)


def finish_kernel(a_ref, b_ref, c_ref, d_ref, g1_ref, g3_ref, g2_ref):
    tops = pl.num_programs(0) - pl.num_programs(0) // 3
    i = pl.program_id(0)
    left = a_ref[...] + b_ref[...]
    right = c_ref[...] + d_ref[...]

    @pl.when(i < tops)
    def _():
        g1_ref[0] = left
        g3_ref[0] = right

    @pl.when(i >= tops)
    def _():
        g2_ref[0] = jnp.concatenate([left, right], axis=1)


def finish(left, late0, right, late1, hidden):
    rows, ff = left.shape
    assert rows == hidden + ff and hidden == 2 * ff
    block = ff // 2
    tops = hidden // block
    top = pl.BlockSpec((1, block, ff), lambda i: (0, jnp.minimum(i, tops - 1), 0))
    return pl.pallas_call(
        finish_kernel,
        grid=(rows // block,),
        out_shape=[jax.ShapeDtypeStruct((1,) + a, F32) for a in ((hidden, ff), (hidden, ff), (ff, hidden))],
        in_specs=[pl.BlockSpec((block, ff), lambda i: (i, 0))] * 4,
        out_specs=[top, top, pl.BlockSpec((1, block, hidden), lambda i: (0, jnp.maximum(i - tops, 0), 0))],
        compiler_params=pltpu.CompilerParams(vmem_limit_bytes=58 * 1024 * 1024),
        cost_estimate=pl.CostEstimate(flops=2 * rows * ff, bytes_accessed=24 * rows * ff, transcendentals=0),
        name='finish',
    )(left, late0, right, late1)


def solution(mesh):
    groups = mesh.shape['grp']
    inner = mesh.shape['ing']
    tok_spec = P(('dp', 'grp', 'ing'), None)
    weight_spec = P(('grp', 'ing'), None, None)
    grad_spec = P(('dp', 'grp', 'ing'), None, None)
    chunks = 2

    def layer(x_loc, ids_loc, gates_loc, dy_loc, wg_loc, wu_loc, wd_loc):
        tokens, hidden = x_loc.shape
        top_k = ids_loc.shape[1]
        per_group = wg_loc.shape[0] * inner
        group_limit = min(max(1, groups // 2), top_k // 2)
        cap = tokens * group_limit // groups
        swap = lambda a: lax.all_to_all(a, 'grp', 0, 0, tiled=True)
        size = cap // chunks
        slot, meta, w_own = make_tables(ids_loc.T, gates_loc.T, (wg_loc, wu_loc, wd_loc), groups, per_group, cap, size)
        w_all = lax.all_gather(w_own, 'ing', axis=0, tiled=True)
        meta = swap(meta)
        recv = []
        for c in range(chunks):
            packed = pack_rows(slot, x_loc, dy_loc, c, size)
            if c == 0:
                packed, slot, meta = lax.optimization_barrier((packed, slot, meta))
            recv.append(swap(packed))
        me = lax.axis_index('ing')
        away = [inner // 2] + [i for i in range(1, inner) if i != inner // 2] + [0]
        order = (me + jnp.asarray(away, jnp.int32)) % inner
        everyone = list(range(per_group))
        ring = lambda a, d: lax.ppermute(a, 'ing', [(i, (i + d) % inner) for i in range(inner)])
        grads = None
        total = None
        c = chunks - 1
        rets = []
        for i in range(c):
            pq, grads = run_experts(i, order, everyone, meta, recv[i], w_all, grads)
            rets.append(swap(pq))
        sums, *far = run_experts(c, order, everyone[:1], meta, recv[c], w_all, grads, None, True)
        far0 = ring(far[0], 1)
        far1 = ring(far[1], -1)
        sums, next0, next1, last0, last1 = run_experts(c, order, everyone[1:-1], meta, recv[c], w_all, grads, sums, True)
        soon1 = ring(next1, 1)
        soon0 = ring(last0, -1)
        pq, own0, own1 = run_experts(c, order, everyone[-1:], meta, recv[c], w_all, grads, sums, False)
        rets.append(swap(pq))
        late0 = ring(next0 + far0, 1)
        late1 = ring(last1 + far1, -1)
        left, right = pair_sums(own0, soon0, own1, soon1)
        for i in range(chunks):
            total = home_sum(slot, rets[i], i, total, i == c, tokens // 4)
            total = total[0] if i < c else total
        y_out, dx_out = total
        g1, g3, g2 = finish(left, late0, right, late1, hidden)
        return y_out, dx_out, g1, g3, g2

    return jax.shard_map(layer, mesh=mesh, in_specs=(tok_spec, tok_spec, tok_spec, tok_spec, weight_spec, weight_spec, weight_spec), out_specs=(tok_spec, tok_spec, grad_spec, grad_spec, grad_spec), check_vma=False)
```
